16 devices in a mesh: dp: 2 (over y, z), sp: 8 (over x, core).
Axes of the slice: x: 4, y: 2, z: 1, core: 2. Of those that a mesh axis runs over, the one named last changes fastest.
The devices are a block of a 4x4x8 slice.
Arguments:
- hidden: bfloat16 [4096, 6144], P(('dp', 'sp')), parts along dimension 0
- w_q: bfloat16 [6144, 6144], replicated
- w_k: bfloat16 [6144, 1024], replicated
- w_v: bfloat16 [6144, 1024], replicated
- w_o: bfloat16 [6144, 6144], replicated
- expert_ids: int32 [4096, 2], P(('dp', 'sp')), parts along dimension 0
- router_probs: float32 [4096, 8], P(('dp', 'sp')), parts along dimension 0
Outputs:
- output 1: bfloat16 [4096, 6144], P(('dp', 'sp')), parts along dimension 0
- output 2: bfloat16 [16, 2048, 6144], P(('dp', 'sp')), parts along dimension 0
There are 2 independent parts. The reference program is written for one: setup_inputs(seed, part) draws one part's arguments, and reference() takes and returns one part's arrays. A program takes and returns all parts, laid end to end along the dimension named above; an argument that names none is the same for every part.
All inputs are finite; a program needn't handle non-finite values.
Results may differ from the reference program's by a relative error of at most 0.00967614.
Values are sent between devices in bfloat16 or wider.
A program may use at most 768 MiB of HBM per device.

```python
import math
import jax
import jax.numpy as jnp
from jax import lax

D = 6144
HEADS = 48
KV_HEADS = 8
HEAD = 128
EXPERTS = 8
TOKENS_DEV = 256
GROUP = 8

SEQ = TOKENS_DEV * GROUP
Q_PER_KV = HEADS // KV_HEADS
Q_WIDTH = HEADS * HEAD
KV_WIDTH = KV_HEADS * HEAD
SCORE_SCALE = 1.0 / math.sqrt(HEAD)


def draw_routes(route_key):
    key_first, key_second, key_pick, key_cold, key_order = jax.random.split(route_key, 5)
    hot_first = jax.random.randint(key_first, (), 0, EXPERTS)
    hot_second = (hot_first + 1 + jax.random.randint(key_second, (), 0, EXPERTS - 1)) % EXPERTS
    pick_hot = jax.random.randint(key_pick, (SEQ,), 0, 2)
    cold_ids = (hot_first + 1 + jax.random.randint(key_cold, (SEQ,), 0, EXPERTS - 1)) % EXPERTS
    other_ids = jnp.where(pick_hot == 1, hot_second, cold_ids)
    first_ids = jnp.full((SEQ,), hot_first)
    swap_bits = jax.random.randint(key_order, (SEQ,), 0, 2)
    col_zero = jnp.where(swap_bits == 1, other_ids, first_ids)
    col_one = jnp.where(swap_bits == 1, first_ids, other_ids)
    return jnp.stack([col_zero, col_one], axis=1).astype(jnp.int32)


def setup_inputs(seed: int = 0, part: int = 0) -> dict:
    base_key = jax.random.key(seed)
    part_key = jax.random.fold_in(base_key, part)
    weight_keys = jax.random.split(base_key, 4)
    part_keys = jax.random.split(part_key, 3)
    q_gain = math.sqrt(0.5 * math.log(SEQ))
    o_gain = 0.5 * SEQ ** 0.25
    hidden = jax.random.normal(part_keys[0], (SEQ, D), jnp.float32).astype(jnp.bfloat16)
    w_q = (jax.random.normal(weight_keys[0], (D, Q_WIDTH), jnp.float32) * (q_gain / math.sqrt(D))).astype(jnp.bfloat16)
    w_k = (jax.random.normal(weight_keys[1], (D, KV_WIDTH), jnp.float32) / math.sqrt(D)).astype(jnp.bfloat16)
    w_v = (jax.random.normal(weight_keys[2], (D, KV_WIDTH), jnp.float32) / math.sqrt(D)).astype(jnp.bfloat16)
    w_o = (jax.random.normal(weight_keys[3], (Q_WIDTH, D), jnp.float32) * (o_gain / math.sqrt(Q_WIDTH))).astype(jnp.bfloat16)
    expert_ids = draw_routes(part_keys[1])
    router_probs = jax.nn.softmax(1.5 * jax.random.normal(part_keys[2], (SEQ, EXPERTS), jnp.float32), axis=1)
    return {'hidden': hidden, 'w_q': w_q, 'w_k': w_k, 'w_v': w_v, 'w_o': w_o, 'expert_ids': expert_ids, 'router_probs': router_probs}


def reference(hidden, w_q, w_k, w_v, w_o, expert_ids, router_probs):
    q_all = jnp.dot(hidden, w_q, preferred_element_type=jnp.float32).astype(jnp.bfloat16)
    k_all = jnp.dot(hidden, w_k, preferred_element_type=jnp.float32).astype(jnp.bfloat16)
    v_all = jnp.dot(hidden, w_v, preferred_element_type=jnp.float32).astype(jnp.bfloat16)
    q_groups = q_all.reshape(SEQ, KV_HEADS, Q_PER_KV, HEAD).transpose(1, 0, 2, 3)
    k_groups = k_all.reshape(SEQ, KV_HEADS, HEAD).transpose(1, 0, 2)
    v_groups = v_all.reshape(SEQ, KV_HEADS, HEAD).transpose(1, 0, 2)
    positions = jnp.arange(SEQ)
    causal = positions[:, None] >= positions[None, :]

    def one_group(group_in):
        q_grp, k_grp, v_grp = group_in
        scores = jnp.einsum('qmd,kd->mqk', q_grp.astype(jnp.float32), k_grp.astype(jnp.float32)) * SCORE_SCALE
        scores = jnp.where(causal[None, :, :], scores, -1e30)
        weights = jax.nn.softmax(scores, axis=-1).astype(jnp.bfloat16)
        out_grp = jnp.einsum('mqk,kd->qmd', weights.astype(jnp.float32), v_grp.astype(jnp.float32))
        return out_grp.astype(jnp.bfloat16)

    attn_out = lax.map(one_group, (q_groups, k_groups, v_groups))
    attn_out = attn_out.transpose(1, 0, 2, 3).reshape(SEQ, Q_WIDTH)
    out_proj = jnp.dot(attn_out, w_o, preferred_element_type=jnp.float32)
    hidden_out = (hidden.astype(jnp.float32) + out_proj).astype(jnp.bfloat16)
    picked = jnp.take_along_axis(router_probs, expert_ids, axis=1)
    gate_w = picked / jnp.sum(picked, axis=1, keepdims=True)
    gated = (gate_w[:, :, None] * hidden_out.astype(jnp.float32)[:, None, :]).astype(jnp.bfloat16)
    ids_blk = expert_ids.reshape(GROUP, TOKENS_DEV, 2)
    token_hits = jnp.sum((ids_blk[:, :, :, None] == jnp.arange(EXPERTS)).astype(jnp.int32), axis=2)
    earlier = jnp.cumsum(token_hits, axis=1) - token_hits
    slot_rank = jnp.take_along_axis(earlier, ids_blk, axis=2)
    dest_rows = jnp.arange(GROUP)[:, None, None] * TOKENS_DEV + slot_rank
    buffer = jnp.zeros((EXPERTS, GROUP * TOKENS_DEV, D), jnp.bfloat16)
    buffer = buffer.at[ids_blk, dest_rows].set(gated.reshape(GROUP, TOKENS_DEV, 2, D))
    return (hidden_out, buffer)
```

```python
import functools
import math
import jax
import jax.numpy as jnp
from jax import lax
from jax.experimental import pallas as pl
from jax.experimental.pallas import tpu as pltpu
from jax.sharding import PartitionSpec as P

HEAD = 128
SCALE = 1.0 / math.sqrt(HEAD)
NEG = -1e30
WIDE = 512
CHUNKS = 4


def attn_kernel(q_ref, k_ref, v_ref, o_ref, m_ref, l_ref, acc_ref):
    me = lax.axis_index('sp')
    rows, width = q_ref.shape
    heads = width // HEAD

    def block(start, size, masked, first):
        k_blk = k_ref[pl.ds(start, size), :]
        v_blk = v_ref[pl.ds(start, size), :]
        for h in range(heads):
            q_h = q_ref[:, h * HEAD:(h + 1) * HEAD]
            s = lax.dot_general(q_h, k_blk, (((1,), (1,)), ((), ())), preferred_element_type=jnp.float32) * SCALE
            if masked:
                r = lax.broadcasted_iota(jnp.int32, s.shape, 0)
                c = lax.broadcasted_iota(jnp.int32, s.shape, 1)
                s = jnp.where(r >= c, s, NEG)
            m_blk = jnp.max(s, axis=1, keepdims=True)
            if first:
                m_new = m_blk
                p = jnp.exp(s - m_new)
                l_ref[h] = jnp.broadcast_to(jnp.sum(p, axis=1, keepdims=True), (rows, HEAD))
                acc_ref[h] = jnp.dot(p.astype(jnp.bfloat16), v_blk, preferred_element_type=jnp.float32)
            else:
                m_old = m_ref[h][:, :1]
                m_new = jnp.maximum(m_old, m_blk)
                p = jnp.exp(s - m_new)
                a = jnp.exp(m_old - m_new)
                l_ref[h] = l_ref[h] * a + jnp.broadcast_to(jnp.sum(p, axis=1, keepdims=True), (rows, HEAD))
                acc_ref[h] = acc_ref[h] * a + jnp.dot(p.astype(jnp.bfloat16), v_blk, preferred_element_type=jnp.float32)
            m_ref[h] = jnp.broadcast_to(m_new, (rows, HEAD))

    block(pl.multiple_of(me * rows, rows), rows, True, True)
    odd = lax.rem(me * rows, WIDE) // rows

    @pl.when(odd == 1)
    def _():
        block(0, rows, False, False)

    @pl.loop(0, (me * rows) // WIDE)
    def _(j):
        block(pl.multiple_of(odd * rows + j * WIDE, rows), WIDE, False, False)

    for h in range(heads):
        o_ref[:, h * HEAD:(h + 1) * HEAD] = (acc_ref[h] / l_ref[h]).astype(o_ref.dtype)


def route_kernel(slot_ref, gate_ref, *refs):
    *h_refs, out_ref = refs
    rows = out_ref.shape[0]
    slot = slot_ref[0]
    r = lax.broadcasted_iota(jnp.int32, (rows, rows), 0)
    pick = slot.astype(jnp.int32) == r
    gate = jnp.sum(jnp.where(pick, gate_ref[0], 0.0), axis=1, keepdims=True)
    pick = jnp.where(pick, 1.0, 0.0).astype(jnp.bfloat16)
    off = 0
    for h_ref in h_refs:
        wid = h_ref.shape[1]
        got = jnp.dot(pick, h_ref[...], preferred_element_type=jnp.float32)
        out_ref[:, off:off + wid] = (gate * got).astype(out_ref.dtype)
        off += wid


def solution(mesh):
    group = mesh.shape['sp']
    row_spec = P(('dp', 'sp'), None)
    buf_spec = P(('dp', 'sp'), None, None)

    def step(x, w_q, w_k, w_v, w_o, ids, probs):
        rows, width = x.shape
        seq = rows * group
        kv_w = w_k.shape[1]
        kv_heads = kv_w // HEAD
        q_w = w_q.shape[1]
        per = q_w // kv_heads
        experts = probs.shape[1]
        hit = jnp.any(ids[:, :, None] == jnp.arange(experts), axis=1)
        picked = jnp.where(hit, probs, 0.0)
        gate = picked / jnp.sum(picked, axis=1, keepdims=True)
        hits = hit.astype(jnp.bfloat16)
        tri = (jnp.arange(rows)[:, None] > jnp.arange(rows)[None, :]).astype(jnp.bfloat16)
        slot = jnp.where(hit, jnp.dot(tri, hits, preferred_element_type=jnp.float32), -1.0)
        table = jnp.stack([slot.T, gate.T], axis=1)
        table = lax.all_to_all(table, 'sp', 0, 0, tiled=True)
        slot_e = table[:, 0:1, :]
        gate_e = table[:, 1:2, :]

        k = jnp.dot(x, w_k, preferred_element_type=jnp.float32).astype(jnp.bfloat16)
        v = jnp.dot(x, w_v, preferred_element_type=jnp.float32).astype(jnp.bfloat16)
        kv = lax.all_gather(jnp.concatenate([k, v], axis=1), 'sp', axis=0, tiled=True)
        q = jnp.dot(x, w_q, preferred_element_type=jnp.float32).astype(jnp.bfloat16)
        o = pl.pallas_call(
            attn_kernel,
            grid=(kv_heads,),
            in_specs=[
                pl.BlockSpec((rows, per), lambda g: (0, g)),
                pl.BlockSpec((seq, HEAD), lambda g: (0, g)),
                pl.BlockSpec((seq, HEAD), lambda g: (0, kv_heads + g)),
            ],
            out_specs=pl.BlockSpec((rows, per), lambda g: (0, g)),
            out_shape=jax.ShapeDtypeStruct((rows, q_w), jnp.bfloat16),
            scratch_shapes=[pltpu.VMEM((per // HEAD, rows, HEAD), jnp.float32)] * 3,
        )(q, kv, kv)
        wid = width // CHUNKS
        parts, gathered = [], []
        for c in range(CHUNKS):
            cols = slice(c * wid, (c + 1) * wid)
            y = jnp.dot(o, w_o[:, cols], preferred_element_type=jnp.float32)
            h_c = (x[:, cols].astype(jnp.float32) + y).astype(jnp.bfloat16)
            parts.append(h_c)
            gathered.append(lax.all_gather(h_c, 'sp', axis=0, tiled=True))
        hidden_out = jnp.concatenate(parts, axis=1)
        buf = pl.pallas_call(
            route_kernel,
            grid=(group,),
            in_specs=[pl.BlockSpec((1, 1, rows), lambda s: (s, 0, 0))] * 2 + [pl.BlockSpec((rows, wid), lambda s: (s, 0))] * CHUNKS,
            out_specs=pl.BlockSpec((rows, width), lambda s: (s, 0)),
            out_shape=jax.ShapeDtypeStruct((seq, width), jnp.bfloat16),
        )(slot_e, gate_e, *gathered)
        return hidden_out, buf[None]

    return jax.shard_map(step, mesh=mesh, in_specs=(row_spec, P(), P(), P(), P(), row_spec, row_spec), out_specs=(row_spec, buf_spec), check_vma=False)
```

```python
import functools
import math
import jax
import jax.numpy as jnp
from jax import lax
from jax.experimental import pallas as pl
from jax.experimental.pallas import tpu as pltpu
from jax.sharding import PartitionSpec as P

HEAD = 128
LOG_SCALE = math.log2(math.e) / math.sqrt(HEAD)
NEG = -1e30
CW = 2 * HEAD
DEPTH = 3
BF16 = jnp.bfloat16
F32 = jnp.float32
MESH = pl.DeviceIdType.MESH


def block_kernel(group, x_ref, wq_ref, wk_ref, wv_ref, wo_ref, tab_ref, h_ref, tabs_ref,
                 q_ref, o_ref, kv_ref, w_ref, m_ref, l_ref, acc_ref,
                 w_sem, x_sem, xs_sem, xr_sem, kvs_sem, kvr_sem, kvf_sem, os_sem, or_sem,
                 hs_sem, hf_sem, hrel_sem, hr_sem, ts_sem, tr_sem):
    me = lax.axis_index('sp')
    chips = group // 2
    chip, core = me // 2, lax.rem(me, 2)
    rows = x_ref.shape[0]
    n_col = x_ref.shape[1] // CW
    half = n_col // 2
    n_kv = wk_ref.shape[1] // HEAD // 2
    per = half // n_kv
    mine = core * half
    sib = chip * 2 + (1 - core)
    right = lax.rem(chip + 1, chips)
    left = lax.rem(chip + chips - 1, chips)
    opp = lax.rem(chip + 2, chips)

    def lane(c):
        return {'sp': c * 2 + core}

    def remote(src, dst, send, recv, dev):
        return pltpu.make_async_remote_copy(src_ref=src, dst_ref=dst, send_sem=send, recv_sem=recv, device_id=dev, device_id_type=MESH)

    n_w = n_kv + 2 * half

    def w_start(i, stage):
        slot = lax.rem(i, DEPTH)
        if stage == 'kv':
            col = pl.multiple_of((core * n_kv + i) * HEAD, HEAD)
            pltpu.make_async_copy(wk_ref.at[:, pl.ds(col, HEAD)], w_ref.at[slot, :, pl.ds(0, HEAD)], w_sem.at[slot, 0]).start()
            pltpu.make_async_copy(wv_ref.at[:, pl.ds(col, HEAD)], w_ref.at[slot, :, pl.ds(HEAD, HEAD)], w_sem.at[slot, 1]).start()
        else:
            src = wq_ref if stage == 'q' else wo_ref
            j = i - n_kv if stage == 'q' else i - n_kv - half
            col = pl.multiple_of((mine + j) * CW, CW)
            pltpu.make_async_copy(src.at[:, pl.ds(col, CW)], w_ref.at[slot], w_sem.at[slot, 0]).start()

    def w_wait(i, stage):
        slot = lax.rem(i, DEPTH)
        if stage == 'kv':
            pltpu.make_async_copy(wk_ref.at[:, pl.ds(0, HEAD)], w_ref.at[slot, :, pl.ds(0, HEAD)], w_sem.at[slot, 0]).wait()
            pltpu.make_async_copy(wv_ref.at[:, pl.ds(0, HEAD)], w_ref.at[slot, :, pl.ds(HEAD, HEAD)], w_sem.at[slot, 1]).wait()
        else:
            pltpu.make_async_copy(wq_ref.at[:, pl.ds(0, CW)], w_ref.at[slot], w_sem.at[slot, 0]).wait()
        return slot

    own_rows = pl.ds(pl.multiple_of(core * rows, rows), rows)
    for j in range(n_col):
        pltpu.make_async_copy(x_ref.at[:, pl.ds(j * CW, CW)], h_ref.at[chip, j, own_rows], x_sem.at[j]).start()
    for i in range(DEPTH):
        w_start(i, 'kv')

    barrier = pltpu.get_barrier_semaphore()
    for d in range(1, group):
        pl.semaphore_signal(barrier, inc=1, device_id={'sp': lax.rem(me + d, group)}, device_id_type=MESH)
    pl.semaphore_wait(barrier, group - 1)

    for j in range(n_col):
        pltpu.make_async_copy(x_ref.at[:, pl.ds(j * CW, CW)], h_ref.at[chip, j, own_rows], x_sem.at[j]).wait()
    x_copy = remote(h_ref.at[chip, :, own_rows], h_ref.at[chip, :, own_rows], xs_sem, xr_sem, {'sp': sib})
    x_copy.start()
    tab_own = pltpu.make_async_copy(tab_ref, tabs_ref.at[me], ts_sem.at[0])
    tab_own.start()
    tab_copies = []
    for d in range(1, group):
        cp = remote(tab_ref, tabs_ref.at[me], ts_sem.at[d], tr_sem.at[d], {'sp': lax.rem(me + d, group)})
        cp.start()
        tab_copies.append(cp)
    x_copy.wait_recv()

    def product(lhs_ref, base, slot):
        lhs = jnp.concatenate([lhs_ref[base, j] for j in range(n_col)], axis=1)
        return jnp.dot(lhs, w_ref[slot], preferred_element_type=F32)

    def kv_own(g, to):
        s = 0 if to == 'r' else 1
        return remote(kv_ref.at[chip, g], kv_ref.at[chip, g], kvs_sem.at[s, g], kvr_sem.at[chip, g], lane(right if to == 'r' else left))

    for g in range(n_kv):
        slot = w_wait(g, 'kv')
        kv_ref[chip, g] = product(h_ref, chip, slot).astype(BF16)
        nxt = g + DEPTH
        w_start(nxt, 'kv' if nxt < n_kv else 'q')
        kv_own(g, 'r').start()
        kv_own(g, 'l').start()

    def kv_in(c, g):
        return remote(kv_ref.at[c, g], kv_ref.at[c, g], kvf_sem.at[g], kvr_sem.at[c, g], lane(right))

    def kv_relay(g):
        kv_in(left, g).wait_recv()
        kv_in(right, g).wait_recv()
        if g < n_kv // 2:
            remote(kv_ref.at[left, g], kv_ref.at[left, g], kvf_sem.at[g], kvr_sem.at[left, g], lane(right)).start()
        else:
            remote(kv_ref.at[right, g], kv_ref.at[right, g], kvf_sem.at[g], kvr_sem.at[right, g], lane(left)).start()

    x_copy.wait_send()
    span = half // n_kv
    for part in range(n_kv):
        @pl.loop(0, span)
        def _(t):
            j = part * span + t
            slot = w_wait(n_kv + j, 'q')
            q_ref[j] = product(h_ref, chip, slot).astype(BF16)
            nxt = n_kv + j + DEPTH

            @pl.when(nxt < n_kv + half)
            def _():
                w_start(nxt, 'q')

            @pl.when(nxt >= n_kv + half)
            def _():
                w_start(nxt, 'o')
        kv_relay(part)

    def attend(g, r):
        n_h = 2 * per
        hb = n_h // 2
        m_rows = hb * rows

        def blk(c, start, size, diag):
            k_blk = kv_ref[c, g, start:start + size, :HEAD]
            v_blk = kv_ref[c, g, start:start + size, HEAD:]
            for u in range(2):
                q_u = jnp.concatenate([q_ref[g * per + (u * hb + i) // 2, r * rows:(r + 1) * rows, ((u * hb + i) % 2) * HEAD:((u * hb + i) % 2 + 1) * HEAD] for i in range(hb)], axis=0)
                s = lax.dot_general(q_u, k_blk, (((1,), (1,)), ((), ())), preferred_element_type=F32)
                if diag:
                    a = lax.broadcasted_iota(jnp.int32, (rows, size), 0) + r * rows
                    b = lax.broadcasted_iota(jnp.int32, (rows, size), 1)
                    s = s + jnp.concatenate([jnp.where(a >= b, 0.0, NEG)] * hb, axis=0)
                cols = [s[:, b * HEAD:(b + 1) * HEAD] for b in range(size // HEAD)]
                mx = functools.reduce(jnp.maximum, cols)
                mx = jnp.broadcast_to(jnp.max(mx, axis=1, keepdims=True), (m_rows, HEAD))
                if not diag:
                    m_old = m_ref[u]
                    mx = jnp.maximum(m_old, mx)
                ps = [jnp.exp2((y - mx) * LOG_SCALE) for y in cols]
                l = functools.reduce(jnp.add, ps)
                pv = jnp.dot(jnp.concatenate([p.astype(BF16) for p in ps], axis=1), v_blk, preferred_element_type=F32)
                if not diag:
                    a = jnp.exp2((m_old - mx) * LOG_SCALE)
                    l = l + l_ref[u] * a
                    pv = pv + acc_ref[u] * a
                m_ref[u] = mx
                l_ref[u] = l
                acc_ref[u] = pv

        blk(chip, 0, (r + 1) * rows, True)

        @pl.loop(0, chip)
        def _(c):
            blk(c, 0, 2 * rows, False)

        for u in range(2):
            o = (acc_ref[u] / jnp.sum(l_ref[u], axis=1, keepdims=True)).astype(BF16)
            for i in range(hb):
                h = u * hb + i
                o_ref[0, mine + g * per + h // 2, r * rows:(r + 1) * rows, (h % 2) * HEAD:(h % 2 + 1) * HEAD] = o[i * rows:(i + 1) * rows]

    def o_copy(g):
        part = o_ref.at[0, pl.ds(mine + g * per, per)]
        return remote(part, part, os_sem.at[g], or_sem.at[g], {'sp': sib})

    def o_in(g):
        part = o_ref.at[0, pl.ds(half - mine + g * per, per)]
        return remote(part, part, os_sem.at[g], or_sem.at[g], {'sp': sib})

    @pl.loop(0, n_kv)
    def _(g):
        @pl.when(g < n_kv // 2)
        def _():
            kv_in(opp, g).wait_recv()

        @pl.when(g >= n_kv // 2)
        def _():
            kv_in(opp, g).wait_recv()
        attend(g, 0)
        attend(g, 1)
        o_copy(g).start()

    for g in range(n_kv):
        o_in(g).wait_recv()

    def h_own(j, k, dev):
        ref = h_ref.at[chip, mine + j]
        return remote(ref, ref, hs_sem.at[k, j], hr_sem.at[chip, mine + j], dev)

    def h_own3(j):
        return (h_own(j, 0, lane(right)), h_own(j, 1, lane(left)), h_own(j, 2, {'sp': sib}))

    @pl.loop(0, half)
    def _(j):
        i = n_kv + half + j
        slot = w_wait(i, 'o')
        y = product(o_ref, 0, slot)
        h_ref[chip, mine + j] = (h_ref[chip, mine + j].astype(F32) + y).astype(BF16)

        @pl.when(i + DEPTH < n_w)
        def _():
            w_start(i + DEPTH, 'o')
        for cp in h_own3(j):
            cp.start()

    first = lax.rem(chip + 1, 2)
    second = first + 2
    base = (chip // 2) * (half // 2)

    def h_fwd(c, k, j):
        ref = h_ref.at[c, mine + j]
        return remote(ref, ref, hf_sem.at[k, j], hr_sem.at[c, mine + j], {'sp': sib})

    def h_relay(c, to, k, t):
        ref = h_ref.at[c, mine + base + t]
        return remote(ref, ref, hrel_sem.at[k, t], hr_sem.at[c, mine + base + t], lane(to))

    for k, (c, to) in enumerate(((first, second), (second, first))):
        @pl.loop(0, half)
        def _(j):
            h_fwd(c, k, j).wait_recv()
            t = j - base

            @pl.when((t >= 0) & (t < half // 2))
            def _():
                h_relay(c, to, k, t).start()
            h_fwd(c, k, j).start()

    @pl.loop(0, half)
    def _(j):
        h_fwd(opp, 2, j).wait_recv()
        h_fwd(opp, 2, j).start()

    def from_sib(c, j):
        ref = h_ref.at[c, half - mine + j]
        return remote(ref, ref, hs_sem.at[0, j], hr_sem.at[c, half - mine + j], {'sp': sib})

    @pl.loop(0, half)
    def _(j):
        for c in range(chips):
            from_sib(c, j).wait_recv()
        for cp in h_own3(j):
            cp.wait_send()
        for k, c in enumerate((first, second, opp)):
            h_fwd(c, k, j).wait_send()

    @pl.loop(0, half // 2)
    def _(t):
        h_relay(first, second, 0, t).wait_send()
        h_relay(second, first, 1, t).wait_send()
    for g in range(n_kv):
        kv_own(g, 'r').wait_send()
        kv_own(g, 'l').wait_send()
        kv_in(left, g).wait_send()
        o_copy(g).wait_send()
    tab_own.wait()
    for cp in tab_copies:
        cp.wait()


def route_kernel(tab_ref, h_ref, buf_ref, out_ref):
    me = lax.axis_index('sp')
    s = pl.program_id(0)
    c = s // 2
    rows = buf_ref.shape[0]
    experts = tab_ref.shape[1] - 8
    tab = tab_ref[s]
    ids = tab[:2].astype(jnp.int32)
    probs = tab[8:]
    exp_row = lax.broadcasted_iota(jnp.int32, (experts, rows), 0)
    hit = jnp.max(jnp.where(ids == me, 1.0, 0.0), axis=0, keepdims=True)
    both = jnp.where((exp_row == ids[0:1]) | (exp_row == ids[1:2]), probs, 0.0)
    p_me = jnp.sum(jnp.where(exp_row == me, probs, 0.0), axis=0, keepdims=True)
    gate = p_me * hit / jnp.sum(both, axis=0, keepdims=True)
    a = lax.broadcasted_iota(jnp.int32, (rows, rows), 0)
    b = lax.broadcasted_iota(jnp.int32, (rows, rows), 1)
    before = jnp.where(a < b, 1.0, 0.0).astype(BF16)
    slot = jnp.dot(jnp.broadcast_to(hit, (8, rows)).astype(BF16), before, preferred_element_type=F32)[:1].astype(jnp.int32)
    pick = (a == slot) & (hit > 0.5)
    g_slot = jnp.sum(jnp.where(pick, gate, 0.0), axis=1, keepdims=True)
    pick = jnp.where(pick, 1.0, 0.0).astype(BF16)
    lo = pl.ds(pl.multiple_of(lax.rem(s, 2) * rows, rows), rows)
    own = s == me
    for j in range(h_ref.shape[1]):
        got = jnp.dot(pick, h_ref[c, j, lo], preferred_element_type=F32)
        buf_ref[:, j * CW:(j + 1) * CW] = (g_slot * got).astype(BF16)

    @pl.when(s == me)
    def _():
        for j in range(h_ref.shape[1]):
            out_ref[:, j * CW:(j + 1) * CW] = h_ref[c, j, lo]


def solution(mesh):
    group = mesh.shape['sp']
    row_spec = P(('dp', 'sp'), None)
    buf_spec = P(('dp', 'sp'), None, None)

    def step(x, w_q, w_k, w_v, w_o, ids, probs):
        rows, width = x.shape
        experts = probs.shape[1]
        chips = group // 2
        n_col = width // CW
        half = n_col // 2
        n_kv = w_k.shape[1] // HEAD // 2
        per = half // n_kv
        crow = 2 * rows
        tab = jnp.concatenate([ids.T.astype(F32), jnp.zeros((6, rows), F32), probs.T], axis=0)
        dma = pltpu.SemaphoreType.DMA
        hbm = pl.BlockSpec(memory_space=pl.ANY)
        vm = pl.BlockSpec(memory_space=pltpu.VMEM)
        h_all, tabs = pl.pallas_call(
            functools.partial(block_kernel, group),
            in_specs=[hbm] * 5 + [vm],
            out_specs=[vm, vm],
            out_shape=[
                pltpu.VMEM((chips, n_col, crow, CW), BF16),
                pltpu.VMEM((group, tab.shape[0], rows), F32),
            ],
            scratch_shapes=[
                pltpu.VMEM((half, crow, CW), BF16),
                pltpu.VMEM((1, n_col, crow, CW), BF16),
                pltpu.VMEM((chips, n_kv, crow, CW), BF16),
                pltpu.VMEM((DEPTH, width, CW), BF16),
                pltpu.VMEM((2, per * rows, HEAD), F32),
                pltpu.VMEM((2, per * rows, HEAD), F32),
                pltpu.VMEM((2, per * rows, HEAD), F32),
                dma((DEPTH, 2)), dma((n_col,)), dma, dma,
                dma((2, n_kv)), dma((chips, n_kv)), dma((n_kv,)), dma((n_kv,)), dma((n_kv,)),
                dma((3, half)), dma((3, half)), dma((2, half // 2)), dma((chips, n_col)),
                dma((group,)), dma((group,)),
            ],
            compiler_params=pltpu.CompilerParams(collective_id=0, has_side_effects=True, vmem_limit_bytes=38 * 1024 * 1024),
        )(x, w_q, w_k, w_v, w_o, tab)
        buf, hidden_out = pl.pallas_call(
            route_kernel,
            grid=(group,),
            in_specs=[vm, vm],
            out_specs=[pl.BlockSpec((rows, width), lambda s: (s, 0)), pl.BlockSpec((rows, width), lambda s: (0, 0))],
            out_shape=[jax.ShapeDtypeStruct((group * rows, width), BF16), jax.ShapeDtypeStruct((rows, width), BF16)],
            compiler_params=pltpu.CompilerParams(vmem_limit_bytes=24 * 1024 * 1024),
        )(pltpu.with_memory_space_constraint(tabs, pltpu.VMEM), pltpu.with_memory_space_constraint(h_all, pltpu.VMEM))
        return hidden_out, buf[None]

    return jax.shard_map(step, mesh=mesh, in_specs=(row_spec, P(), P(), P(), P(), row_spec, row_spec), out_specs=(row_spec, buf_spec), check_vma=False)
```

```python
import functools
import math
import jax
import jax.numpy as jnp
from jax import lax
from jax.experimental import pallas as pl
from jax.experimental.pallas import tpu as pltpu
from jax.sharding import PartitionSpec as P

HEAD = 128
LOG_SCALE = math.log2(math.e) / math.sqrt(HEAD)
NEG = -1e30
CW = 2 * HEAD
DEPTH = 4
SHARE = 7
BF16 = jnp.bfloat16
F32 = jnp.float32
MESH = pl.DeviceIdType.MESH


def block_kernel(group, x_ref, wq_ref, wk_ref, wv_ref, wo_ref, tab_ref, h_ref, tabs_ref,
                 xs_ref, q_ref, o_ref, kv_ref, w_ref, hs_ref, m_ref, l_ref, acc_ref,
                 w_sem, x_sem, xs_sem, xr_sem, kvs_sem, kvr_sem, kvf_sem, os_sem, or_sem,
                 hs_sem, hf_sem, hrel_sem, hr_sem, ts_sem, tr_sem):
    me = lax.axis_index('sp')
    chips = group // 2
    chip, core = me // 2, lax.rem(me, 2)
    rows = x_ref.shape[0]
    n_col = x_ref.shape[1] // CW
    half = n_col // 2
    n_kv = wk_ref.shape[1] // HEAD // 2
    per = half // n_kv
    mine = core * half
    sib = chip * 2 + (1 - core)
    right = lax.rem(chip + 1, chips)
    left = lax.rem(chip + chips - 1, chips)
    opp = lax.rem(chip + 2, chips)

    def lane(c):
        return {'sp': c * 2 + core}

    def remote(src, dst, send, recv, dev):
        return pltpu.make_async_remote_copy(src_ref=src, dst_ref=dst, send_sem=send, recv_sem=recv, device_id=dev, device_id_type=MESH)

    n_w = n_kv + 4 * half

    def w_start(i, stage):
        slot = lax.rem(i, DEPTH)
        if stage == 'kv':
            col = pl.multiple_of((core * n_kv + i) * HEAD, HEAD)
            pltpu.make_async_copy(wk_ref.at[:, pl.ds(col, HEAD)], w_ref.at[slot, :, pl.ds(0, HEAD)], w_sem.at[slot, 0]).start()
            pltpu.make_async_copy(wv_ref.at[:, pl.ds(col, HEAD)], w_ref.at[slot, :, pl.ds(HEAD, HEAD)], w_sem.at[slot, 1]).start()
        else:
            src = wq_ref if stage == 'q' else wo_ref
            j = lax.rem(i - n_kv, half)
            col = pl.multiple_of((mine + j) * CW, CW)
            pltpu.make_async_copy(src.at[:, pl.ds(col, CW)], w_ref.at[slot], w_sem.at[slot, 0]).start()

    def w_wait(i, stage):
        slot = lax.rem(i, DEPTH)
        if stage == 'kv':
            pltpu.make_async_copy(wk_ref.at[:, pl.ds(0, HEAD)], w_ref.at[slot, :, pl.ds(0, HEAD)], w_sem.at[slot, 0]).wait()
            pltpu.make_async_copy(wv_ref.at[:, pl.ds(0, HEAD)], w_ref.at[slot, :, pl.ds(HEAD, HEAD)], w_sem.at[slot, 1]).wait()
        else:
            pltpu.make_async_copy(wq_ref.at[:, pl.ds(0, CW)], w_ref.at[slot], w_sem.at[slot, 0]).wait()
        return slot

    own_rows = pl.ds(pl.multiple_of(core * rows, rows), rows)
    for j in range(n_col):
        pltpu.make_async_copy(x_ref.at[:, pl.ds(j * CW, CW)], xs_ref.at[j, own_rows], x_sem.at[j]).start()
    for i in range(DEPTH):
        w_start(i, 'kv' if i < n_kv else 'q')

    barrier = pltpu.get_barrier_semaphore()
    for d in range(1, group):
        pl.semaphore_signal(barrier, inc=1, device_id={'sp': lax.rem(me + d, group)}, device_id_type=MESH)
    pl.semaphore_wait(barrier, group - 1)

    for j in range(n_col):
        pltpu.make_async_copy(x_ref.at[:, pl.ds(j * CW, CW)], xs_ref.at[j, own_rows], x_sem.at[j]).wait()
    x_copy = remote(xs_ref.at[:, own_rows], xs_ref.at[:, own_rows], xs_sem, xr_sem, {'sp': sib})
    x_copy.start()
    tab_own = pltpu.make_async_copy(tab_ref, tabs_ref.at[me], ts_sem.at[0])
    tab_own.start()
    tab_copies = []
    for d in range(1, group):
        cp = remote(tab_ref, tabs_ref.at[me], ts_sem.at[d], tr_sem.at[d], {'sp': lax.rem(me + d, group)})
        cp.start()
        tab_copies.append(cp)
    x_copy.wait_recv()

    def product(lhs_ref, slot):
        lhs = jnp.concatenate([lhs_ref[j] for j in range(n_col)], axis=1)
        return jnp.dot(lhs, w_ref[slot], preferred_element_type=F32)

    def kv_own(g, to):
        s = 0 if to == 'r' else 1
        return remote(kv_ref.at[chip, g], kv_ref.at[chip, g], kvs_sem.at[s, g], kvr_sem.at[chip, g], lane(right if to == 'r' else left))

    for g in range(n_kv):
        slot = w_wait(g, 'kv')
        kv_ref[chip, g] = product(xs_ref, slot).astype(BF16)
        nxt = g + DEPTH
        w_start(nxt, 'kv' if nxt < n_kv else 'q')
        kv_own(g, 'r').start()
        kv_own(g, 'l').start()

    def kv_in(c, g):
        return remote(kv_ref.at[c, g], kv_ref.at[c, g], kvf_sem.at[g], kvr_sem.at[c, g], lane(right))

    def kv_relay(g):
        kv_in(left, g).wait_recv()
        kv_in(right, g).wait_recv()
        if g < n_kv // 2:
            remote(kv_ref.at[left, g], kv_ref.at[left, g], kvf_sem.at[g], kvr_sem.at[left, g], lane(right)).start()
        else:
            remote(kv_ref.at[right, g], kv_ref.at[right, g], kvf_sem.at[g], kvr_sem.at[right, g], lane(left)).start()

    def w_next(i):
        nxt = i + DEPTH
        lap = (nxt - n_kv) // half

        @pl.when((nxt < n_w) & (lax.rem(lap, 2) == 0))
        def _():
            w_start(nxt, 'q')

        @pl.when((nxt < n_w) & (lax.rem(lap, 2) == 1))
        def _():
            w_start(nxt, 'o')

    def queries(r, lo, n):
        @pl.loop(lo, lo + n)
        def _(j):
            i = n_kv + 2 * r * half + j
            slot = w_wait(i, 'q')
            q_ref[j] = product(xs_ref.at[:, r * rows:(r + 1) * rows], slot).astype(BF16)
            w_next(i)

    span = half // n_kv
    for part in range(n_kv):
        queries(0, part * span, span)
        if part < n_kv - 1:
            kv_relay(part)

    n_h = 2 * per
    hb = n_h // 2
    m_rows = hb * rows

    def blk(g, r, c, size, diag):
        k_blk = kv_ref[c, g, :size, :HEAD]
        v_blk = kv_ref[c, g, :size, HEAD:]
        scores = []
        for u in range(2):
            q_u = jnp.concatenate([q_ref[g * per + (u * hb + i) // 2, :, ((u * hb + i) % 2) * HEAD:((u * hb + i) % 2 + 1) * HEAD] for i in range(hb)], axis=0)
            scores.append(lax.dot_general(q_u, k_blk, (((1,), (1,)), ((), ())), preferred_element_type=F32))
        for u in range(2):
            s = scores[u]
            if diag:
                a = lax.broadcasted_iota(jnp.int32, (rows, size), 0) + r * rows
                b = lax.broadcasted_iota(jnp.int32, (rows, size), 1)
                s = s + jnp.concatenate([jnp.where(a >= b, 0.0, NEG)] * hb, axis=0)
            cols = [s[:, b * HEAD:(b + 1) * HEAD] for b in range(size // HEAD)]
            mx = functools.reduce(jnp.maximum, cols)
            mx = jnp.broadcast_to(jnp.max(mx, axis=1, keepdims=True), (m_rows, HEAD))
            if not diag:
                m_old = m_ref[g, u]
                mx = jnp.maximum(m_old, mx)
            ps = [jnp.exp2((y - mx) * LOG_SCALE) for y in cols]
            l = functools.reduce(jnp.add, ps)
            pv = jnp.dot(jnp.concatenate([p.astype(BF16) for p in ps], axis=1), v_blk, preferred_element_type=F32)
            if not diag:
                a = jnp.exp2((m_old - mx) * LOG_SCALE)
                l = l + l_ref[g, u] * a
                pv = pv + acc_ref[g, u] * a
            m_ref[g, u] = mx
            l_ref[g, u] = l
            acc_ref[g, u] = pv

    def finish(g, r):
        for u in range(2):
            o = (acc_ref[g, u] / jnp.sum(l_ref[g, u], axis=1, keepdims=True)).astype(BF16)
            for i in range(hb):
                h = u * hb + i
                o_ref[r, mine + g * per + h // 2, :, (h % 2) * HEAD:(h % 2 + 1) * HEAD] = o[i * rows:(i + 1) * rows]

    def o_copy(r, g):
        part = o_ref.at[r, pl.ds(mine + g * per, per)]
        return remote(part, part, os_sem.at[r, g], or_sem.at[r, g], {'sp': sib})

    def o_in(r, g):
        part = o_ref.at[r, pl.ds(half - mine + g * per, per)]
        return remote(part, part, os_sem.at[r, g], or_sem.at[r, g], {'sp': sib})

    def piece(s, j):
        return h_ref.at[pl.ds(pl.multiple_of(s * rows, rows), rows), pl.ds(pl.multiple_of(j * CW, CW), CW)]

    def h_own(r, j, k, dev):
        s = chip * 2 + r
        return remote(hs_ref.at[r, j], piece(s, mine + j), hs_sem.at[k, r, j], hr_sem.at[s, mine + j], dev)

    def h_own3(r, j):
        return (h_own(r, j, 0, lane(right)), h_own(r, j, 1, lane(left)), h_own(r, j, 2, {'sp': sib}))

    def h_keep(r, j):
        return pltpu.make_async_copy(hs_ref.at[r, j], piece(chip * 2 + r, mine + j), hs_sem.at[3, r, j])

    def project(r):
        @pl.loop(0, half)
        def _(j):
            i = n_kv + (1 + 2 * r) * half + j
            slot = w_wait(i, 'o')
            y = product(o_ref.at[r], slot)
            hs_ref[r, j] = (xs_ref[mine + j, r * rows:(r + 1) * rows].astype(F32) + y).astype(BF16)

            w_next(i)
            for cp in h_own3(r, j):
                cp.start()
            h_keep(r, j).start()

    first = lax.rem(chip + 1, 2)
    second = first + 2
    early = chip < chips // 2

    def h_fwd(c, r, k, j):
        ref = piece(c * 2 + r, mine + j)
        return remote(ref, ref, hf_sem.at[k, r, j], hr_sem.at[c * 2 + r, mine + j], {'sp': sib})

    def h_relay(c, to, r, k, j):
        ref = piece(c * 2 + r, mine + j)
        return remote(ref, ref, hrel_sem.at[k, r, j], hr_sem.at[c * 2 + r, mine + j], lane(to))

    cut = half * SHARE // 12

    def relayed(j):
        return early == (j < cut)

    def relay(k, r):
        c, to = ((first, second), (second, first))[k]

        @pl.loop(0, half)
        def _(j):
            h_fwd(c, r, k, j).wait_recv()

            @pl.when(relayed(j))
            def _():
                h_relay(c, to, r, k, j).start()
            h_fwd(c, r, k, j).start()

    late, last = chip >= chips // 2, chip == chips - 1
    for r in range(2):
        if r == 1:
            queries(1, 0, half)

        @pl.loop(0, n_kv)
        def _(g):
            if r == 0:
                pl.when(g == 1)(lambda: kv_relay(n_kv - 1))
            else:
                pl.when((g == 1) & late)(lambda: relay(0, 0))
                pl.when((g == 2) & last)(lambda: relay(1, 0))
            blk(g, r, chip, (r + 1) * rows, True)

            @pl.loop(0, 2)
            def _(n):
                c = n * right + (1 - n) * left

                @pl.when(c < chip)
                def _():
                    blk(g, r, c, 2 * rows, False)

        @pl.loop(0, n_kv)
        def _(g):
            if r == 0:
                kv_in(opp, g).wait_recv()

            @pl.when(opp < chip)
            def _():
                blk(g, r, opp, 2 * rows, False)
            finish(g, r)
            o_copy(r, g).start()
        for g in range(n_kv):
            o_in(r, g).wait_recv()
        project(r)

    pl.when(jnp.logical_not(late))(lambda: relay(0, 0))
    pl.when(jnp.logical_not(last))(lambda: relay(1, 0))
    relay(0, 1)
    relay(1, 1)
    for r in range(2):
        @pl.loop(0, half)
        def _(j):
            h_fwd(opp, r, 2, j).wait_recv()
            h_fwd(opp, r, 2, j).start()

    def from_sib(c, r, j):
        ref = piece(c * 2 + r, half - mine + j)
        return remote(ref, ref, hs_sem.at[0, r, j], hr_sem.at[c * 2 + r, half - mine + j], {'sp': sib})

    for r in range(2):
        @pl.loop(0, half)
        def _(j):
            for c in range(chips):
                from_sib(c, r, j).wait_recv()
            for cp in h_own3(r, j):
                cp.wait_send()
            h_keep(r, j).wait()
            for k, c in enumerate((first, second, opp)):
                h_fwd(c, r, k, j).wait_send()

            @pl.when(relayed(j))
            def _():
                h_relay(first, second, r, 0, j).wait_send()
                h_relay(second, first, r, 1, j).wait_send()
    for g in range(n_kv):
        kv_own(g, 'r').wait_send()
        kv_own(g, 'l').wait_send()
        kv_in(left, g).wait_send()
        for r in range(2):
            o_copy(r, g).wait_send()
    x_copy.wait_send()
    tab_own.wait()
    for cp in tab_copies:
        cp.wait()


def route_kernel(tab_ref, h_ref, buf_ref, out_ref):
    me = lax.axis_index('sp')
    s = pl.program_id(0)
    rows = buf_ref.shape[0]
    experts = tab_ref.shape[1] - 8
    tab = tab_ref[0]
    ids = tab[:2].astype(jnp.int32)
    probs = tab[8:]
    exp_row = lax.broadcasted_iota(jnp.int32, (experts, rows), 0)
    hit = jnp.max(jnp.where(ids == me, 1.0, 0.0), axis=0, keepdims=True)
    both = jnp.where((exp_row == ids[0:1]) | (exp_row == ids[1:2]), probs, 0.0)
    p_me = jnp.sum(jnp.where(exp_row == me, probs, 0.0), axis=0, keepdims=True)
    gate = p_me * hit / jnp.sum(both, axis=0, keepdims=True)
    a = lax.broadcasted_iota(jnp.int32, (rows, rows), 0)
    b = lax.broadcasted_iota(jnp.int32, (rows, rows), 1)
    before = jnp.where(a < b, 1.0, 0.0).astype(BF16)
    slot = jnp.dot(jnp.broadcast_to(hit, (8, rows)).astype(BF16), before, preferred_element_type=F32)[:1].astype(jnp.int32)
    pick = (a == slot) & (hit > 0.5)
    g_slot = jnp.sum(jnp.where(pick, gate, 0.0), axis=1, keepdims=True)
    pick = jnp.where(pick, 1.0, 0.0).astype(BF16)
    for j in range(buf_ref.shape[1] // CW):
        cols = slice(j * CW, (j + 1) * CW)
        got = jnp.dot(pick, h_ref[:, cols], preferred_element_type=F32)
        buf_ref[:, cols] = (g_slot * got).astype(BF16)

    @pl.when(s == me)
    def _():
        out_ref[...] = h_ref[...]


def solution(mesh):
    group = mesh.shape['sp']
    row_spec = P(('dp', 'sp'), None)
    buf_spec = P(('dp', 'sp'), None, None)

    def step(x, w_q, w_k, w_v, w_o, ids, probs):
        rows, width = x.shape
        experts = probs.shape[1]
        chips = group // 2
        n_col = width // CW
        half = n_col // 2
        n_kv = w_k.shape[1] // HEAD // 2
        per = half // n_kv
        crow = 2 * rows
        tab = jnp.concatenate([ids.T.astype(F32), jnp.zeros((6, rows), F32), probs.T], axis=0)
        dma = pltpu.SemaphoreType.DMA
        hbm = pl.BlockSpec(memory_space=pl.ANY)
        vm = pl.BlockSpec(memory_space=pltpu.VMEM)
        h_all, tabs = pl.pallas_call(
            functools.partial(block_kernel, group),
            in_specs=[hbm] * 5 + [vm],
            out_specs=[hbm, hbm],
            out_shape=[
                jax.ShapeDtypeStruct((group * rows, width), BF16),
                jax.ShapeDtypeStruct((group, tab.shape[0], rows), F32),
            ],
            scratch_shapes=[
                pltpu.VMEM((n_col, crow, CW), BF16),
                pltpu.VMEM((half, rows, CW), BF16),
                pltpu.VMEM((2, n_col, rows, CW), BF16),
                pltpu.VMEM((chips, n_kv, crow, CW), BF16),
                pltpu.VMEM((DEPTH, width, CW), BF16),
                pltpu.VMEM((2, half, rows, CW), BF16),
                pltpu.VMEM((n_kv, 2, per * rows, HEAD), F32),
                pltpu.VMEM((n_kv, 2, per * rows, HEAD), F32),
                pltpu.VMEM((n_kv, 2, per * rows, HEAD), F32),
                dma((DEPTH, 2)), dma((n_col,)), dma, dma,
                dma((2, n_kv)), dma((chips, n_kv)), dma((n_kv,)), dma((2, n_kv)), dma((2, n_kv)),
                dma((4, 2, half)), dma((3, 2, half)), dma((2, 2, half)), dma((group, n_col)),
                dma((group,)), dma((group,)),
            ],
            compiler_params=pltpu.CompilerParams(collective_id=0, has_side_effects=True, vmem_limit_bytes=56 * 1024 * 1024),
        )(x, w_q, w_k, w_v, w_o, tab)
        buf, hidden_out = pl.pallas_call(
            route_kernel,
            grid=(group,),
            in_specs=[pl.BlockSpec((1, tab.shape[0], rows), lambda s: (s, 0, 0)), pl.BlockSpec((rows, width), lambda s: (s, 0))],
            out_specs=[pl.BlockSpec((rows, width), lambda s: (s, 0)), pl.BlockSpec((rows, width), lambda s: (0, 0))],
            out_shape=[jax.ShapeDtypeStruct((group * rows, width), BF16), jax.ShapeDtypeStruct((rows, width), BF16)],
        )(tabs, h_all)
        return hidden_out, buf[None]

    return jax.shard_map(step, mesh=mesh, in_specs=(row_spec, P(), P(), P(), P(), row_spec, row_spec), out_specs=(row_spec, buf_spec), check_vma=False)
```

```python
import functools
import math
import jax
import jax.numpy as jnp
from jax import lax
from jax.experimental import pallas as pl
from jax.experimental.pallas import tpu as pltpu
from jax.sharding import PartitionSpec as P

HEAD = 128
LOG_SCALE = math.log2(math.e) / math.sqrt(HEAD)
NEG = -1e30
CW = 2 * HEAD
DEPTH = 4
SHARE = 7
AHEAD = 4
SLOTS = 4
BF16 = jnp.bfloat16
F32 = jnp.float32
MESH = pl.DeviceIdType.MESH


def block_kernel(group, x_ref, wq_ref, wk_ref, wv_ref, wo_ref, tab_ref, h_ref, tabs_ref,
                 xs_ref, q_ref, o_ref, ks_ref, kv_ref, w_ref, hs_ref, m_ref, l_ref, acc_ref,
                 w_sem, x_sem, xs_sem, xr_sem, kvs_sem, kvr_sem, kvf_sem, os_sem, or_sem,
                 hs_sem, hf_sem, hrel_sem, hr_sem, ts_sem, tr_sem):
    me = lax.axis_index('sp')
    chips = group // 2
    chip, core = me // 2, lax.rem(me, 2)
    rows = x_ref.shape[0]
    n_col = x_ref.shape[1] // CW
    half = n_col // 2
    n_kv = wk_ref.shape[1] // HEAD // 2
    per = half // n_kv
    mine = core * half
    sib = chip * 2 + (1 - core)
    right = lax.rem(chip + 1, chips)
    left = lax.rem(chip + chips - 1, chips)
    opp = lax.rem(chip + 2, chips)

    def lane(c):
        return {'sp': c * 2 + core}

    def remote(src, dst, send, recv, dev):
        return pltpu.make_async_remote_copy(src_ref=src, dst_ref=dst, send_sem=send, recv_sem=recv, device_id=dev, device_id_type=MESH)

    n_k = 2 * n_kv
    n_w = n_k + 4 * half

    def w_start(i, stage):
        slot = lax.rem(jnp.int32(i), DEPTH)
        if stage == 'kv':
            col = (i % 2 * n_kv + i // 2) * HEAD
            pltpu.make_async_copy(wk_ref.at[:, pl.ds(col, HEAD)], w_ref.at[slot, :, pl.ds(0, HEAD)], w_sem.at[slot, 0]).start()
            pltpu.make_async_copy(wv_ref.at[:, pl.ds(col, HEAD)], w_ref.at[slot, :, pl.ds(HEAD, HEAD)], w_sem.at[slot, 1]).start()
        else:
            src = wq_ref if stage == 'q' else wo_ref
            j = lax.rem(i - n_k, half)
            col = pl.multiple_of((mine + j) * CW, CW)
            pltpu.make_async_copy(src.at[:, pl.ds(col, CW)], w_ref.at[slot], w_sem.at[slot, 0]).start()

    def w_wait(i, stage):
        slot = lax.rem(jnp.int32(i), DEPTH)
        if stage == 'kv':
            pltpu.make_async_copy(wk_ref.at[:, pl.ds(0, HEAD)], w_ref.at[slot, :, pl.ds(0, HEAD)], w_sem.at[slot, 0]).wait()
            pltpu.make_async_copy(wv_ref.at[:, pl.ds(0, HEAD)], w_ref.at[slot, :, pl.ds(HEAD, HEAD)], w_sem.at[slot, 1]).wait()
        else:
            pltpu.make_async_copy(wq_ref.at[:, pl.ds(0, CW)], w_ref.at[slot], w_sem.at[slot, 0]).wait()
        return slot

    own_rows = pl.ds(pl.multiple_of(core * rows, rows), rows)
    for j in range(n_col):
        pltpu.make_async_copy(x_ref.at[:, pl.ds(j * CW, CW)], xs_ref.at[j, own_rows], x_sem.at[j]).start()
    for i in range(DEPTH):
        w_start(i, 'kv' if i < n_k else 'q')

    barrier = pltpu.get_barrier_semaphore()
    for d in range(1, group):
        pl.semaphore_signal(barrier, inc=1, device_id={'sp': lax.rem(me + d, group)}, device_id_type=MESH)

    for j in range(n_col):
        pltpu.make_async_copy(x_ref.at[:, pl.ds(j * CW, CW)], xs_ref.at[j, own_rows], x_sem.at[j]).wait()
    x_copy = remote(xs_ref.at[:, own_rows], xs_ref.at[:, own_rows], xs_sem, xr_sem, {'sp': sib})
    tab_own = pltpu.make_async_copy(tab_ref, tabs_ref.at[me], ts_sem.at[0])
    tab_copies = [remote(tab_ref, tabs_ref.at[me], ts_sem.at[d], tr_sem.at[d], {'sp': lax.rem(me + d, group)}) for d in range(1, group)]

    def product(lhs_ref, slot):
        lhs = jnp.concatenate([lhs_ref[j] for j in range(n_col)], axis=1)
        return jnp.dot(lhs, w_ref[slot], preferred_element_type=F32)

    def kv_own(i, k):
        ln, g = i % 2, i // 2
        dev = (right * 2 + ln, left * 2 + ln, sib)[k]
        return remote(ks_ref.at[ln, g], kv_ref.at[chip, g, own_rows], kvs_sem.at[k, i], kvr_sem.at[chip, g, core], {'sp': dev})

    for i in range(n_k):
        slot = w_wait(i, 'kv')
        kv = product(xs_ref.at[:, own_rows], slot).astype(BF16)
        ks_ref[i % 2, i // 2] = kv

        @pl.when(core == i % 2)
        def _():
            kv_ref[chip, i // 2, own_rows] = kv
        w_start(i + DEPTH, 'kv' if i + DEPTH < n_k else 'q')
        if i == 0:
            pl.semaphore_wait(barrier, group - 1)
            x_copy.start()
        kv_own(i, 0).start()
        kv_own(i, 1).start()
        pl.when(core != i % 2)(kv_own(i, 2).start)
    tab_own.start()
    for cp in tab_copies:
        cp.start()

    def kv_part(c, g, b, to):
        ref = kv_ref.at[c, g, pl.ds(b * rows, rows)]
        return remote(ref, ref, kvf_sem.at[g, b], kvr_sem.at[c, g, b], lane(to))

    def kv_wait(c, g):
        kv_part(c, g, 0, right).wait_recv()
        kv_part(c, g, 1, right).wait_recv()

    def kv_relay(g):
        kv_wait(left, g)
        kv_wait(right, g)
        for b in range(2):
            if g < n_kv // 2:
                kv_part(left, g, b, right).start()
            else:
                kv_part(right, g, b, left).start()

    x_copy.wait_recv()
    x_copy.wait_send()
    def w_next(i):
        nxt = i + DEPTH
        lap = (nxt - n_k) // half

        @pl.when((nxt < n_w) & (lax.rem(lap, 2) == 0))
        def _():
            w_start(nxt, 'q')

        @pl.when((nxt < n_w) & (lax.rem(lap, 2) == 1))
        def _():
            w_start(nxt, 'o')

    def queries(r, lo, n):
        @pl.loop(lo, lo + n)
        def _(j):
            i = n_k + 2 * r * half + j
            slot = w_wait(i, 'q')
            q_ref[j] = product(xs_ref.at[:, r * rows:(r + 1) * rows], slot).astype(BF16)
            w_next(i)

    span = half // n_kv
    for part in range(n_kv):
        queries(0, part * span, span)
        if part < n_kv - 1:
            kv_relay(part)

    n_h = 2 * per
    hb = n_h // 2
    m_rows = hb * rows

    def blk(g, r, c, size, diag):
        k_blk = kv_ref[c, g, :size, :HEAD]
        v_blk = kv_ref[c, g, :size, HEAD:]
        scores = []
        for u in range(2):
            q_u = jnp.concatenate([q_ref[g * per + (u * hb + i) // 2, :, ((u * hb + i) % 2) * HEAD:((u * hb + i) % 2 + 1) * HEAD] for i in range(hb)], axis=0)
            scores.append(lax.dot_general(q_u, k_blk, (((1,), (1,)), ((), ())), preferred_element_type=F32))
        for u in range(2):
            s = scores[u]
            if diag:
                a = lax.broadcasted_iota(jnp.int32, (rows, size), 0) + r * rows
                b = lax.broadcasted_iota(jnp.int32, (rows, size), 1)
                s = s + jnp.concatenate([jnp.where(a >= b, 0.0, NEG)] * hb, axis=0)
            cols = [s[:, b * HEAD:(b + 1) * HEAD] for b in range(size // HEAD)]
            mx = functools.reduce(jnp.maximum, cols)
            mx = jnp.broadcast_to(jnp.max(mx, axis=1, keepdims=True), (m_rows, HEAD))
            if not diag:
                m_old = m_ref[g, u]
                mx = jnp.maximum(m_old, mx)
            ps = [jnp.exp2((y - mx) * LOG_SCALE) for y in cols]
            l = functools.reduce(jnp.add, ps)
            pv = jnp.dot(jnp.concatenate([p.astype(BF16) for p in ps], axis=1), v_blk, preferred_element_type=F32)
            if not diag:
                a = jnp.exp2((m_old - mx) * LOG_SCALE)
                l = l + l_ref[g, u] * a
                pv = pv + acc_ref[g, u] * a
            m_ref[g, u] = mx
            l_ref[g, u] = l
            acc_ref[g, u] = pv

    def finish(g, r):
        for u in range(2):
            o = (acc_ref[g, u] / jnp.sum(l_ref[g, u], axis=1, keepdims=True)).astype(BF16)
            for i in range(hb):
                h = u * hb + i
                o_ref[r, mine + g * per + h // 2, :, (h % 2) * HEAD:(h % 2 + 1) * HEAD] = o[i * rows:(i + 1) * rows]

    def o_copy(r, g):
        part = o_ref.at[r, pl.ds(mine + g * per, per)]
        return remote(part, part, os_sem.at[r, g], or_sem.at[r, g], {'sp': sib})

    def o_in(r, g):
        part = o_ref.at[r, pl.ds(half - mine + g * per, per)]
        return remote(part, part, os_sem.at[r, g], or_sem.at[r, g], {'sp': sib})

    def piece(s, j):
        return h_ref.at[pl.ds(pl.multiple_of(s * rows, rows), rows), pl.ds(pl.multiple_of(j * CW, CW), CW)]

    def h_own(r, j, k, dev):
        s = chip * 2 + r
        return remote(hs_ref.at[r, j], piece(s, mine + j), hs_sem.at[k, r, j], hr_sem.at[s, mine + j], dev)

    def h_own3(r, j):
        return (h_own(r, j, 0, lane(right)), h_own(r, j, 1, lane(left)), h_own(r, j, 2, {'sp': sib}))

    def h_keep(r, j):
        return pltpu.make_async_copy(hs_ref.at[r, j], piece(chip * 2 + r, mine + j), hs_sem.at[3, r, j])

    def project(r):
        @pl.loop(0, half)
        def _(j):
            i = n_k + (1 + 2 * r) * half + j
            slot = w_wait(i, 'o')
            y = product(o_ref.at[r], slot)
            hs_ref[r, j] = (xs_ref[mine + j, r * rows:(r + 1) * rows].astype(F32) + y).astype(BF16)

            w_next(i)
            for cp in h_own3(r, j):
                cp.start()
            h_keep(r, j).start()

    first = lax.rem(chip + 1, 2)
    second = first + 2
    early = chip < chips // 2

    def h_fwd(c, r, k, j):
        ref = piece(c * 2 + r, mine + j)
        return remote(ref, ref, hf_sem.at[k, r, j], hr_sem.at[c * 2 + r, mine + j], {'sp': sib})

    def h_relay(c, to, r, k, j):
        ref = piece(c * 2 + r, mine + j)
        return remote(ref, ref, hrel_sem.at[k, r, j], hr_sem.at[c * 2 + r, mine + j], lane(to))

    cut = half * SHARE // 12

    def relayed(j):
        return early == (j < cut)

    def relay(k, r):
        c, to = ((first, second), (second, first))[k]

        @pl.loop(0, half)
        def _(j):
            h_fwd(c, r, k, j).wait_recv()

            @pl.when(relayed(j))
            def _():
                h_relay(c, to, r, k, j).start()
            h_fwd(c, r, k, j).start()

    late, last = chip >= chips // 2, chip == chips - 1
    for r in range(2):
        if r == 1:
            queries(1, 0, half)

        @pl.loop(0, n_kv)
        def _(g):
            if r == 0:
                pl.when(g == 1)(lambda: kv_relay(n_kv - 1))
                kv_part(chip, g, 1 - core, right).wait_recv()
            else:
                pl.when((g == 1) & late)(lambda: relay(0, 0))
                pl.when((g == 2) & last)(lambda: relay(1, 0))
            blk(g, r, chip, (r + 1) * rows, True)

            @pl.loop(0, 2)
            def _(n):
                c = n * right + (1 - n) * left

                @pl.when(c < chip)
                def _():
                    blk(g, r, c, 2 * rows, False)

        @pl.loop(0, n_kv)
        def _(g):
            if r == 0:
                kv_wait(opp, g)

            @pl.when(opp < chip)
            def _():
                blk(g, r, opp, 2 * rows, False)
            finish(g, r)
            o_copy(r, g).start()
        for g in range(n_kv):
            o_in(r, g).wait_recv()
        project(r)

    pl.when(jnp.logical_not(late))(lambda: relay(0, 0))
    pl.when(jnp.logical_not(last))(lambda: relay(1, 0))
    relay(0, 1)
    relay(1, 1)
    for r in range(2):
        @pl.loop(0, half)
        def _(j):
            h_fwd(opp, r, 2, j).wait_recv()
            h_fwd(opp, r, 2, j).start()

    def from_sib(c, r, j):
        ref = piece(c * 2 + r, half - mine + j)
        return remote(ref, ref, hs_sem.at[0, r, j], hr_sem.at[c * 2 + r, half - mine + j], {'sp': sib})

    for r in range(2):
        @pl.loop(0, half)
        def _(j):
            for c in range(chips):
                from_sib(c, r, j).wait_recv()
            for cp in h_own3(r, j):
                cp.wait_send()
            h_keep(r, j).wait()
            for k, c in enumerate((first, second, opp)):
                h_fwd(c, r, k, j).wait_send()

            @pl.when(relayed(j))
            def _():
                h_relay(first, second, r, 0, j).wait_send()
                h_relay(second, first, r, 1, j).wait_send()
    for i in range(n_k):
        kv_own(i, 0).wait_send()
        kv_own(i, 1).wait_send()
        pl.when(core != i % 2)(kv_own(i, 2).wait_send)
    for g in range(n_kv):
        for b in range(2):
            kv_part(left, g, b, right).wait_send()
            o_copy(b, g).wait_send()
    tab_own.wait()
    for cp in tab_copies:
        cp.wait()


def route_kernel(group, tab_ref, h_ref, buf_ref, out_ref, in_ref, st_ref, in_sem, st_sem, own_sem):
    me = lax.axis_index('sp')
    rows, width = out_ref.shape
    experts = tab_ref.shape[1] - 8
    exp_row = lax.broadcasted_iota(jnp.int32, (experts, rows), 0)
    a = lax.broadcasted_iota(jnp.int32, (rows, rows), 0)
    b = lax.broadcasted_iota(jnp.int32, (rows, rows), 1)
    before = jnp.where(a < b, 1.0, 0.0).astype(BF16)

    def fetch(s):
        return pltpu.make_async_copy(h_ref.at[pl.ds(s * rows, rows)], in_ref.at[s], in_sem.at[s])

    def put(s):
        return pltpu.make_async_copy(st_ref.at[s % SLOTS], buf_ref.at[pl.ds(s * rows, rows)], st_sem.at[s])

    own = pltpu.make_async_copy(in_ref.at[me], out_ref, own_sem)
    for s in range(AHEAD):
        fetch(s).start()
    for s in range(group):
        tab = tab_ref[s]
        ids = tab[:2].astype(jnp.int32)
        probs = tab[8:]
        hit = jnp.max(jnp.where(ids == me, 1.0, 0.0), axis=0, keepdims=True)
        both = jnp.where((exp_row == ids[0:1]) | (exp_row == ids[1:2]), probs, 0.0)
        p_me = jnp.sum(jnp.where(exp_row == me, probs, 0.0), axis=0, keepdims=True)
        gate = p_me * hit / jnp.sum(both, axis=0, keepdims=True)
        slot = jnp.dot(jnp.broadcast_to(hit, (8, rows)).astype(BF16), before, preferred_element_type=F32)[:1].astype(jnp.int32)
        pick = (a == slot) & (hit > 0.5)
        g_slot = jnp.broadcast_to(jnp.sum(jnp.where(pick, gate, 0.0), axis=1, keepdims=True), (rows, CW))
        pick = jnp.where(pick, 1.0, 0.0).astype(BF16)
        fetch(s).wait()
        if s + AHEAD < group:
            fetch(s + AHEAD).start()
        if s >= SLOTS:
            put(s - SLOTS).wait()
        for j in range(width // CW):
            cols = slice(j * CW, (j + 1) * CW)
            got = jnp.dot(pick, in_ref[s, :, cols], preferred_element_type=F32)
            st_ref[s % SLOTS, :, cols] = (g_slot * got).astype(BF16)
        put(s).start()
    own.start()
    for s in range(group - SLOTS, group):
        put(s).wait()
    own.wait()


def solution(mesh):
    group = mesh.shape['sp']
    row_spec = P(('dp', 'sp'), None)
    buf_spec = P(('dp', 'sp'), None, None)

    def step(x, w_q, w_k, w_v, w_o, ids, probs):
        rows, width = x.shape
        experts = probs.shape[1]
        chips = group // 2
        n_col = width // CW
        half = n_col // 2
        n_kv = w_k.shape[1] // HEAD // 2
        per = half // n_kv
        crow = 2 * rows
        tab = jnp.concatenate([ids.T.astype(F32), jnp.zeros((6, rows), F32), probs.T], axis=0)
        dma = pltpu.SemaphoreType.DMA
        hbm = pl.BlockSpec(memory_space=pl.ANY)
        vm = pl.BlockSpec(memory_space=pltpu.VMEM)
        h_all, tabs = pl.pallas_call(
            functools.partial(block_kernel, group),
            in_specs=[hbm] * 5 + [vm],
            out_specs=[hbm, hbm],
            out_shape=[
                jax.ShapeDtypeStruct((group * rows, width), BF16),
                jax.ShapeDtypeStruct((group, tab.shape[0], rows), F32),
            ],
            scratch_shapes=[
                pltpu.VMEM((n_col, crow, CW), BF16),
                pltpu.VMEM((half, rows, CW), BF16),
                pltpu.VMEM((2, n_col, rows, CW), BF16),
                pltpu.VMEM((2, n_kv, rows, CW), BF16),
                pltpu.VMEM((chips, n_kv, crow, CW), BF16),
                pltpu.VMEM((DEPTH, width, CW), BF16),
                pltpu.VMEM((2, half, rows, CW), BF16),
                pltpu.VMEM((n_kv, 2, per * rows, HEAD), F32),
                pltpu.VMEM((n_kv, 2, per * rows, HEAD), F32),
                pltpu.VMEM((n_kv, 2, per * rows, HEAD), F32),
                dma((DEPTH, 2)), dma((n_col,)), dma, dma,
                dma((3, 2 * n_kv)), dma((chips, n_kv, 2)), dma((n_kv, 2)), dma((2, n_kv)), dma((2, n_kv)),
                dma((4, 2, half)), dma((3, 2, half)), dma((2, 2, half)), dma((group, n_col)),
                dma((group,)), dma((group,)),
            ],
            compiler_params=pltpu.CompilerParams(collective_id=0, has_side_effects=True, vmem_limit_bytes=56 * 1024 * 1024),
        )(x, w_q, w_k, w_v, w_o, tab)
        buf, hidden_out = pl.pallas_call(
            functools.partial(route_kernel, group),
            in_specs=[vm, hbm],
            out_specs=[hbm, hbm],
            out_shape=[jax.ShapeDtypeStruct((group * rows, width), BF16), jax.ShapeDtypeStruct((rows, width), BF16)],
            scratch_shapes=[
                pltpu.VMEM((group, rows, width), BF16),
                pltpu.VMEM((SLOTS, rows, width), BF16),
                dma((group,)), dma((group,)), dma,
            ],
            compiler_params=pltpu.CompilerParams(vmem_limit_bytes=56 * 1024 * 1024),
        )(tabs, h_all)
        return hidden_out, buf[None]

    return jax.shard_map(step, mesh=mesh, in_specs=(row_spec, P(), P(), P(), P(), row_spec, row_spec), out_specs=(row_spec, buf_spec), check_vma=False)
```

```python
import functools
import math
import jax
import jax.numpy as jnp
from jax import lax
from jax.experimental import pallas as pl
from jax.experimental.pallas import tpu as pltpu
from jax.sharding import PartitionSpec as P

HEAD = 128
LOG_SCALE = math.log2(math.e) / math.sqrt(HEAD)
NEG = -1e30
CW = 2 * HEAD
DEPTH = 4
SHARE = 7
AHEAD = 4
SLOTS = 4
BF16 = jnp.bfloat16
F32 = jnp.float32
MESH = pl.DeviceIdType.MESH


def block_kernel(group, x_ref, wq_ref, wk_ref, wv_ref, wo_ref, tab_ref, h_ref, tabs_ref,
                 xs_ref, q_ref, o_ref, ks_ref, kv_ref, w_ref, hs_ref, m_ref, l_ref, acc_ref,
                 w_sem, x_sem, xs_sem, xr_sem, kvs_sem, kvr_sem, kvf_sem, os_sem, or_sem,
                 hs_sem, hf_sem, hrel_sem, hr_sem, ts_sem, tr_sem):
    me = lax.axis_index('sp')
    chips = group // 2
    chip, core = me // 2, lax.rem(me, 2)
    rows = x_ref.shape[0]
    n_col = x_ref.shape[1] // CW
    half = n_col // 2
    n_kv = wk_ref.shape[1] // HEAD // 2
    per = half // n_kv
    mine = core * half
    sib = chip * 2 + (1 - core)
    right = lax.rem(chip + 1, chips)
    left = lax.rem(chip + chips - 1, chips)
    opp = lax.rem(chip + 2, chips)

    def lane(c):
        return {'sp': c * 2 + core}

    def remote(src, dst, send, recv, dev):
        return pltpu.make_async_remote_copy(src_ref=src, dst_ref=dst, send_sem=send, recv_sem=recv, device_id=dev, device_id_type=MESH)

    n_k = 2 * n_kv
    n_w = n_k + 4 * half

    def w_start(i, stage):
        slot = lax.rem(jnp.int32(i), DEPTH)
        if stage == 'kv':
            col = (i % 2 * n_kv + i // 2) * HEAD
            pltpu.make_async_copy(wk_ref.at[:, pl.ds(col, HEAD)], w_ref.at[slot, :, pl.ds(0, HEAD)], w_sem.at[slot, 0]).start()
            pltpu.make_async_copy(wv_ref.at[:, pl.ds(col, HEAD)], w_ref.at[slot, :, pl.ds(HEAD, HEAD)], w_sem.at[slot, 1]).start()
        else:
            src = wq_ref if stage == 'q' else wo_ref
            j = lax.rem(i - n_k, half)
            col = pl.multiple_of((mine + j) * CW, CW)
            pltpu.make_async_copy(src.at[:, pl.ds(col, CW)], w_ref.at[slot], w_sem.at[slot, 0]).start()

    def w_wait(i, stage):
        slot = lax.rem(jnp.int32(i), DEPTH)
        if stage == 'kv':
            pltpu.make_async_copy(wk_ref.at[:, pl.ds(0, HEAD)], w_ref.at[slot, :, pl.ds(0, HEAD)], w_sem.at[slot, 0]).wait()
            pltpu.make_async_copy(wv_ref.at[:, pl.ds(0, HEAD)], w_ref.at[slot, :, pl.ds(HEAD, HEAD)], w_sem.at[slot, 1]).wait()
        else:
            pltpu.make_async_copy(wq_ref.at[:, pl.ds(0, CW)], w_ref.at[slot], w_sem.at[slot, 0]).wait()
        return slot

    own_rows = pl.ds(pl.multiple_of(core * rows, rows), rows)
    for j in range(n_col):
        pltpu.make_async_copy(x_ref.at[:, pl.ds(j * CW, CW)], xs_ref.at[j, own_rows], x_sem.at[j]).start()
    for i in range(DEPTH):
        w_start(i, 'kv' if i < n_k else 'q')

    barrier = pltpu.get_barrier_semaphore()
    for d in range(1, group):
        pl.semaphore_signal(barrier, inc=1, device_id={'sp': lax.rem(me + d, group)}, device_id_type=MESH)

    for j in range(n_col):
        pltpu.make_async_copy(x_ref.at[:, pl.ds(j * CW, CW)], xs_ref.at[j, own_rows], x_sem.at[j]).wait()
    x_copy = remote(xs_ref.at[:, own_rows], xs_ref.at[:, own_rows], xs_sem, xr_sem, {'sp': sib})
    tab_own = pltpu.make_async_copy(tab_ref, tabs_ref.at[me], ts_sem.at[0])
    tab_copies = [remote(tab_ref, tabs_ref.at[me], ts_sem.at[d], tr_sem.at[d], {'sp': lax.rem(me + d, group)}) for d in range(1, group)]

    def product(lhs_ref, slot):
        lhs = jnp.concatenate([lhs_ref[j] for j in range(n_col)], axis=1)
        return jnp.dot(lhs, w_ref[slot], preferred_element_type=F32)

    def kv_own(i, k):
        ln, g = i % 2, i // 2
        dev = (right * 2 + ln, left * 2 + ln, sib)[k]
        return remote(ks_ref.at[ln, g], kv_ref.at[chip, g, own_rows], kvs_sem.at[k, i], kvr_sem.at[chip, g, core], {'sp': dev})

    def to_right(c, low):
        return (lax.rem(c + 1, chips) > c) | (low & (lax.rem(c + 2, chips) > c))

    def to_left(c, low):
        return (lax.rem(c + chips - 1, chips) > c) | (jnp.logical_not(low) & (lax.rem(c + 2, chips) > c))

    def low_head(g):
        return jnp.bool_(g < n_kv // 2)

    def kv_sent(i, act):
        low = low_head(i // 2)
        pl.when(to_right(chip, low))(lambda: act(kv_own(i, 0)))
        pl.when(to_left(chip, low))(lambda: act(kv_own(i, 1)))
        pl.when(core != i % 2)(lambda: act(kv_own(i, 2)))

    for i in range(n_k):
        slot = w_wait(i, 'kv')
        kv = product(xs_ref.at[:, own_rows], slot).astype(BF16)
        ks_ref[i % 2, i // 2] = kv

        @pl.when(core == i % 2)
        def _():
            kv_ref[chip, i // 2, own_rows] = kv
        w_start(i + DEPTH, 'kv' if i + DEPTH < n_k else 'q')
        if i == 0:
            pl.semaphore_wait(barrier, group - 1)
            x_copy.start()
        kv_sent(i, lambda cp: cp.start())
    tab_own.start()
    for cp in tab_copies:
        cp.start()

    def kv_part(c, g, b, to):
        ref = kv_ref.at[c, g, pl.ds(b * rows, rows)]
        return remote(ref, ref, kvf_sem.at[g, b], kvr_sem.at[c, g, b], lane(to))

    def kv_wait(c, g):
        kv_part(c, g, 0, right).wait_recv()
        kv_part(c, g, 1, right).wait_recv()

    def kv_passed(g, act):
        c, to = (left, right) if g < n_kv // 2 else (right, left)

        @pl.when(to > c)
        def _():
            for b in range(2):
                act(kv_part(c, g, b, to))

    def kv_relay(g):
        low = low_head(g)
        pl.when(to_right(left, low))(lambda: kv_wait(left, g))
        pl.when(to_left(right, low))(lambda: kv_wait(right, g))
        kv_passed(g, lambda cp: cp.start())

    x_copy.wait_recv()
    x_copy.wait_send()
    def w_next(i):
        nxt = i + DEPTH
        lap = (nxt - n_k) // half

        @pl.when((nxt < n_w) & (lax.rem(lap, 2) == 0))
        def _():
            w_start(nxt, 'q')

        @pl.when((nxt < n_w) & (lax.rem(lap, 2) == 1))
        def _():
            w_start(nxt, 'o')

    def queries(r, lo, n):
        @pl.loop(lo, lo + n)
        def _(j):
            i = n_k + 2 * r * half + j
            slot = w_wait(i, 'q')
            q_ref[j] = product(xs_ref.at[:, r * rows:(r + 1) * rows], slot).astype(BF16)
            w_next(i)

    span = half // n_kv
    for part in range(n_kv):
        queries(0, part * span, span)
        if part < n_kv - 1:
            kv_relay(part)

    n_h = 2 * per
    hb = n_h // 2
    m_rows = hb * rows

    def blk(g, r, c, size, diag):
        k_blk = kv_ref[c, g, :size, :HEAD]
        v_blk = kv_ref[c, g, :size, HEAD:]
        scores = []
        for u in range(2):
            q_u = jnp.concatenate([q_ref[g * per + (u * hb + i) // 2, :, ((u * hb + i) % 2) * HEAD:((u * hb + i) % 2 + 1) * HEAD] for i in range(hb)], axis=0)
            scores.append(lax.dot_general(q_u, k_blk, (((1,), (1,)), ((), ())), preferred_element_type=F32))
        for u in range(2):
            s = scores[u]
            if diag:
                a = lax.broadcasted_iota(jnp.int32, (rows, size), 0) + r * rows
                b = lax.broadcasted_iota(jnp.int32, (rows, size), 1)
                s = s + jnp.concatenate([jnp.where(a >= b, 0.0, NEG)] * hb, axis=0)
            cols = [s[:, b * HEAD:(b + 1) * HEAD] for b in range(size // HEAD)]
            mx = functools.reduce(jnp.maximum, cols)
            mx = jnp.broadcast_to(jnp.max(mx, axis=1, keepdims=True), (m_rows, HEAD))
            if not diag:
                m_old = m_ref[g, u]
                mx = jnp.maximum(m_old, mx)
            ps = [jnp.exp2((y - mx) * LOG_SCALE) for y in cols]
            l = functools.reduce(jnp.add, ps)
            pv = jnp.dot(jnp.concatenate([p.astype(BF16) for p in ps], axis=1), v_blk, preferred_element_type=F32)
            if not diag:
                a = jnp.exp2((m_old - mx) * LOG_SCALE)
                l = l + l_ref[g, u] * a
                pv = pv + acc_ref[g, u] * a
            m_ref[g, u] = mx
            l_ref[g, u] = l
            acc_ref[g, u] = pv

    def finish(g, r):
        for u in range(2):
            o = (acc_ref[g, u] / jnp.sum(l_ref[g, u], axis=1, keepdims=True)).astype(BF16)
            for i in range(hb):
                h = u * hb + i
                o_ref[r, mine + g * per + h // 2, :, (h % 2) * HEAD:(h % 2 + 1) * HEAD] = o[i * rows:(i + 1) * rows]

    def o_copy(r, g):
        part = o_ref.at[r, pl.ds(mine + g * per, per)]
        return remote(part, part, os_sem.at[r, g], or_sem.at[r, g], {'sp': sib})

    def o_in(r, g):
        part = o_ref.at[r, pl.ds(half - mine + g * per, per)]
        return remote(part, part, os_sem.at[r, g], or_sem.at[r, g], {'sp': sib})

    def piece(s, j):
        return h_ref.at[pl.ds(pl.multiple_of(s * rows, rows), rows), pl.ds(pl.multiple_of(j * CW, CW), CW)]

    def h_own(r, j, k, dev):
        s = chip * 2 + r
        return remote(hs_ref.at[r, j], piece(s, mine + j), hs_sem.at[k, r, j], hr_sem.at[s, mine + j], dev)

    def h_own3(r, j):
        return (h_own(r, j, 0, lane(right)), h_own(r, j, 1, lane(left)), h_own(r, j, 2, {'sp': sib}))

    def h_keep(r, j):
        return pltpu.make_async_copy(hs_ref.at[r, j], piece(chip * 2 + r, mine + j), hs_sem.at[3, r, j])

    def project(r):
        @pl.loop(0, half)
        def _(j):
            i = n_k + (1 + 2 * r) * half + j
            slot = w_wait(i, 'o')
            y = product(o_ref.at[r], slot)
            hs_ref[r, j] = (xs_ref[mine + j, r * rows:(r + 1) * rows].astype(F32) + y).astype(BF16)

            w_next(i)
            for cp in h_own3(r, j):
                cp.start()
            h_keep(r, j).start()

    first = lax.rem(chip + 1, 2)
    second = first + 2
    early = chip < chips // 2

    def h_fwd(c, r, k, j):
        ref = piece(c * 2 + r, mine + j)
        return remote(ref, ref, hf_sem.at[k, r, j], hr_sem.at[c * 2 + r, mine + j], {'sp': sib})

    def h_relay(c, to, r, k, j):
        ref = piece(c * 2 + r, mine + j)
        return remote(ref, ref, hrel_sem.at[k, r, j], hr_sem.at[c * 2 + r, mine + j], lane(to))

    cut = half * SHARE // 12

    def relayed(j):
        return early == (j < cut)

    def relay(k, r):
        c, to = ((first, second), (second, first))[k]

        @pl.loop(0, half)
        def _(j):
            h_fwd(c, r, k, j).wait_recv()

            @pl.when(relayed(j))
            def _():
                h_relay(c, to, r, k, j).start()
            h_fwd(c, r, k, j).start()

    late, last = chip >= chips // 2, chip == chips - 1
    for r in range(2):
        if r == 1:
            queries(1, 0, half)

        @pl.loop(0, n_kv)
        def _(g):
            if r == 0:
                pl.when(g == 1)(lambda: kv_relay(n_kv - 1))
                kv_part(chip, g, 1 - core, right).wait_recv()
            else:
                pl.when((g == 2) & late)(lambda: relay(0, 0))
                pl.when((g == 3) & last)(lambda: relay(1, 0))
            blk(g, r, chip, (r + 1) * rows, True)

            @pl.loop(0, 2)
            def _(n):
                c = n * right + (1 - n) * left

                @pl.when(c < chip)
                def _():
                    blk(g, r, c, 2 * rows, False)

        @pl.loop(0, n_kv)
        def _(g):
            @pl.when(opp < chip)
            def _():
                if r == 0:
                    kv_wait(opp, g)
                blk(g, r, opp, 2 * rows, False)
            finish(g, r)
            o_copy(r, g).start()
        for g in range(n_kv):
            o_in(r, g).wait_recv()
        project(r)

    pl.when(jnp.logical_not(late))(lambda: relay(0, 0))
    pl.when(jnp.logical_not(last))(lambda: relay(1, 0))
    relay(0, 1)
    relay(1, 1)
    for r in range(2):
        @pl.loop(0, half)
        def _(j):
            h_fwd(opp, r, 2, j).wait_recv()
            h_fwd(opp, r, 2, j).start()

    def from_sib(c, r, j):
        ref = piece(c * 2 + r, half - mine + j)
        return remote(ref, ref, hs_sem.at[0, r, j], hr_sem.at[c * 2 + r, half - mine + j], {'sp': sib})

    for r in range(2):
        @pl.loop(0, half)
        def _(j):
            for c in range(chips):
                from_sib(c, r, j).wait_recv()
            for cp in h_own3(r, j):
                cp.wait_send()
            h_keep(r, j).wait()
            for k, c in enumerate((first, second, opp)):
                h_fwd(c, r, k, j).wait_send()

            @pl.when(relayed(j))
            def _():
                h_relay(first, second, r, 0, j).wait_send()
                h_relay(second, first, r, 1, j).wait_send()
    for i in range(n_k):
        kv_sent(i, lambda cp: cp.wait_send())
    for g in range(n_kv):
        kv_passed(g, lambda cp: cp.wait_send())
        for b in range(2):
            o_copy(b, g).wait_send()
    tab_own.wait()
    for cp in tab_copies:
        cp.wait()


def route_kernel(group, tab_ref, h_ref, buf_ref, out_ref, in_ref, st_ref, in_sem, st_sem, own_sem):
    me = lax.axis_index('sp')
    rows, width = out_ref.shape
    experts = tab_ref.shape[1] - 8
    exp_row = lax.broadcasted_iota(jnp.int32, (experts, rows), 0)
    a = lax.broadcasted_iota(jnp.int32, (rows, rows), 0)
    b = lax.broadcasted_iota(jnp.int32, (rows, rows), 1)
    before = jnp.where(a < b, 1.0, 0.0).astype(BF16)

    def fetch(s):
        return pltpu.make_async_copy(h_ref.at[pl.ds(s * rows, rows)], in_ref.at[s], in_sem.at[s])

    def put(s):
        return pltpu.make_async_copy(st_ref.at[s % SLOTS], buf_ref.at[pl.ds(s * rows, rows)], st_sem.at[s])

    own = pltpu.make_async_copy(in_ref.at[me], out_ref, own_sem)
    for s in range(AHEAD):
        fetch(s).start()
    for s in range(group):
        tab = tab_ref[s]
        ids = tab[:2].astype(jnp.int32)
        probs = tab[8:]
        hit = jnp.max(jnp.where(ids == me, 1.0, 0.0), axis=0, keepdims=True)
        both = jnp.where((exp_row == ids[0:1]) | (exp_row == ids[1:2]), probs, 0.0)
        p_me = jnp.sum(jnp.where(exp_row == me, probs, 0.0), axis=0, keepdims=True)
        gate = p_me * hit / jnp.sum(both, axis=0, keepdims=True)
        slot = jnp.dot(jnp.broadcast_to(hit, (8, rows)).astype(BF16), before, preferred_element_type=F32)[:1].astype(jnp.int32)
        pick = (a == slot) & (hit > 0.5)
        g_slot = jnp.broadcast_to(jnp.sum(jnp.where(pick, gate, 0.0), axis=1, keepdims=True), (rows, CW))
        pick = jnp.where(pick, 1.0, 0.0).astype(BF16)
        fetch(s).wait()
        if s + AHEAD < group:
            fetch(s + AHEAD).start()
        if s >= SLOTS:
            put(s - SLOTS).wait()
        for j in range(width // CW):
            cols = slice(j * CW, (j + 1) * CW)
            got = jnp.dot(pick, in_ref[s, :, cols], preferred_element_type=F32)
            st_ref[s % SLOTS, :, cols] = (g_slot * got).astype(BF16)
        put(s).start()
    own.start()
    for s in range(group - SLOTS, group):
        put(s).wait()
    own.wait()


def solution(mesh):
    group = mesh.shape['sp']
    row_spec = P(('dp', 'sp'), None)
    buf_spec = P(('dp', 'sp'), None, None)

    def step(x, w_q, w_k, w_v, w_o, ids, probs):
        rows, width = x.shape
        experts = probs.shape[1]
        chips = group // 2
        n_col = width // CW
        half = n_col // 2
        n_kv = w_k.shape[1] // HEAD // 2
        per = half // n_kv
        crow = 2 * rows
        tab = jnp.concatenate([ids.T.astype(F32), jnp.zeros((6, rows), F32), probs.T], axis=0)
        dma = pltpu.SemaphoreType.DMA
        hbm = pl.BlockSpec(memory_space=pl.ANY)
        vm = pl.BlockSpec(memory_space=pltpu.VMEM)
        h_all, tabs = pl.pallas_call(
            functools.partial(block_kernel, group),
            in_specs=[hbm] * 5 + [vm],
            out_specs=[hbm, hbm],
            out_shape=[
                jax.ShapeDtypeStruct((group * rows, width), BF16),
                jax.ShapeDtypeStruct((group, tab.shape[0], rows), F32),
            ],
            scratch_shapes=[
                pltpu.VMEM((n_col, crow, CW), BF16),
                pltpu.VMEM((half, rows, CW), BF16),
                pltpu.VMEM((2, n_col, rows, CW), BF16),
                pltpu.VMEM((2, n_kv, rows, CW), BF16),
                pltpu.VMEM((chips, n_kv, crow, CW), BF16),
                pltpu.VMEM((DEPTH, width, CW), BF16),
                pltpu.VMEM((2, half, rows, CW), BF16),
                pltpu.VMEM((n_kv, 2, per * rows, HEAD), F32),
                pltpu.VMEM((n_kv, 2, per * rows, HEAD), F32),
                pltpu.VMEM((n_kv, 2, per * rows, HEAD), F32),
                dma((DEPTH, 2)), dma((n_col,)), dma, dma,
                dma((3, 2 * n_kv)), dma((chips, n_kv, 2)), dma((n_kv, 2)), dma((2, n_kv)), dma((2, n_kv)),
                dma((4, 2, half)), dma((3, 2, half)), dma((2, 2, half)), dma((group, n_col)),
                dma((group,)), dma((group,)),
            ],
            compiler_params=pltpu.CompilerParams(collective_id=0, has_side_effects=True, vmem_limit_bytes=56 * 1024 * 1024),
        )(x, w_q, w_k, w_v, w_o, tab)
        buf, hidden_out = pl.pallas_call(
            functools.partial(route_kernel, group),
            in_specs=[vm, hbm],
            out_specs=[hbm, hbm],
            out_shape=[jax.ShapeDtypeStruct((group * rows, width), BF16), jax.ShapeDtypeStruct((rows, width), BF16)],
            scratch_shapes=[
                pltpu.VMEM((group, rows, width), BF16),
                pltpu.VMEM((SLOTS, rows, width), BF16),
                dma((group,)), dma((group,)), dma,
            ],
            compiler_params=pltpu.CompilerParams(vmem_limit_bytes=56 * 1024 * 1024),
        )(tabs, h_all)
        return hidden_out, buf[None]

    return jax.shard_map(step, mesh=mesh, in_specs=(row_spec, P(), P(), P(), P(), row_spec, row_spec), out_specs=(row_spec, buf_spec), check_vma=False)
```

```python
import functools
import math
import jax
import jax.numpy as jnp
from jax import lax
from jax.experimental import pallas as pl
from jax.experimental.pallas import tpu as pltpu
from jax.sharding import PartitionSpec as P

HEAD = 128
LOG_SCALE = math.log2(math.e) / math.sqrt(HEAD)
NEG = -1e30
CW = 2 * HEAD
DEPTH = 4
SHARE = 7
AHEAD = 4
SLOTS = 4
BF16 = jnp.bfloat16
F32 = jnp.float32
MESH = pl.DeviceIdType.MESH


def block_kernel(group, x_ref, wq_ref, wk_ref, wv_ref, wo_ref, tab_ref, h_ref, tabs_ref,
                 xs_ref, q_ref, o_ref, ks_ref, kv_ref, w_ref, hs_ref, m_ref, l_ref, acc_ref,
                 w_sem, x_sem, xs_sem, xr_sem, kvs_sem, kvr_sem, kvf_sem, os_sem, or_sem,
                 hs_sem, hf_sem, hrel_sem, hr_sem, ts_sem, tr_sem):
    me = lax.axis_index('sp')
    chips = group // 2
    chip, core = me // 2, lax.rem(me, 2)
    rows = x_ref.shape[0]
    n_col = x_ref.shape[1] // CW
    half = n_col // 2
    n_kv = wk_ref.shape[1] // HEAD // 2
    per = half // n_kv
    mine = core * half
    sib = chip * 2 + (1 - core)
    right = lax.rem(chip + 1, chips)
    left = lax.rem(chip + chips - 1, chips)
    opp = lax.rem(chip + 2, chips)

    def lane(c):
        return {'sp': c * 2 + core}

    def remote(src, dst, send, recv, dev):
        return pltpu.make_async_remote_copy(src_ref=src, dst_ref=dst, send_sem=send, recv_sem=recv, device_id=dev, device_id_type=MESH)

    n_k = 2 * n_kv
    n_w = n_k + 4 * half

    def w_start(i, stage):
        slot = lax.rem(jnp.int32(i), DEPTH)
        if stage == 'kv':
            col = (i % 2 * n_kv + i // 2) * HEAD
            pltpu.make_async_copy(wk_ref.at[:, pl.ds(col, HEAD)], w_ref.at[slot, :, pl.ds(0, HEAD)], w_sem.at[slot, 0]).start()
            pltpu.make_async_copy(wv_ref.at[:, pl.ds(col, HEAD)], w_ref.at[slot, :, pl.ds(HEAD, HEAD)], w_sem.at[slot, 1]).start()
        else:
            src = wq_ref if stage == 'q' else wo_ref
            j = lax.rem(i - n_k, half)
            col = pl.multiple_of((mine + j) * CW, CW)
            pltpu.make_async_copy(src.at[:, pl.ds(col, CW)], w_ref.at[slot], w_sem.at[slot, 0]).start()

    def w_wait(i, stage):
        slot = lax.rem(jnp.int32(i), DEPTH)
        if stage == 'kv':
            pltpu.make_async_copy(wk_ref.at[:, pl.ds(0, HEAD)], w_ref.at[slot, :, pl.ds(0, HEAD)], w_sem.at[slot, 0]).wait()
            pltpu.make_async_copy(wv_ref.at[:, pl.ds(0, HEAD)], w_ref.at[slot, :, pl.ds(HEAD, HEAD)], w_sem.at[slot, 1]).wait()
        else:
            pltpu.make_async_copy(wq_ref.at[:, pl.ds(0, CW)], w_ref.at[slot], w_sem.at[slot, 0]).wait()
        return slot

    own_rows = pl.ds(pl.multiple_of(core * rows, rows), rows)
    for j in range(n_col):
        pltpu.make_async_copy(x_ref.at[:, pl.ds(j * CW, CW)], xs_ref.at[j, own_rows], x_sem.at[j]).start()
    w_start(0, 'kv')

    barrier = pltpu.get_barrier_semaphore()
    for d in range(1, group):
        pl.semaphore_signal(barrier, inc=1, device_id={'sp': lax.rem(me + d, group)}, device_id_type=MESH)

    for j in range(n_col):
        pltpu.make_async_copy(x_ref.at[:, pl.ds(j * CW, CW)], xs_ref.at[j, own_rows], x_sem.at[j]).wait()
    for i in range(1, DEPTH):
        w_start(i, 'kv' if i < n_k else 'q')
    x_copy = remote(xs_ref.at[:, own_rows], xs_ref.at[:, own_rows], xs_sem, xr_sem, {'sp': sib})
    tab_own = pltpu.make_async_copy(tab_ref, tabs_ref.at[me], ts_sem.at[0])
    tab_copies = [remote(tab_ref, tabs_ref.at[me], ts_sem.at[d], tr_sem.at[d], {'sp': lax.rem(me + d, group)}) for d in range(1, group)]

    def product(lhs_ref, slot):
        lhs = jnp.concatenate([lhs_ref[j] for j in range(n_col)], axis=1)
        return jnp.dot(lhs, w_ref[slot], preferred_element_type=F32)

    def kv_own(i, k):
        ln, g = i % 2, i // 2
        dev = (right * 2 + ln, left * 2 + ln, sib)[k]
        return remote(ks_ref.at[ln, g], kv_ref.at[chip, g, own_rows], kvs_sem.at[k, i], kvr_sem.at[chip, g, core], {'sp': dev})

    def to_right(c, low):
        return (lax.rem(c + 1, chips) > c) | (low & (lax.rem(c + 2, chips) > c))

    def to_left(c, low):
        return (lax.rem(c + chips - 1, chips) > c) | (jnp.logical_not(low) & (lax.rem(c + 2, chips) > c))

    def low_head(g):
        return jnp.bool_(g < n_kv // 2)

    def kv_sent(i, act):
        low = low_head(i // 2)
        pl.when(to_right(chip, low))(lambda: act(kv_own(i, 0)))
        pl.when(to_left(chip, low))(lambda: act(kv_own(i, 1)))
        pl.when(core != i % 2)(lambda: act(kv_own(i, 2)))

    for i in range(n_k):
        slot = w_wait(i, 'kv')
        kv = product(xs_ref.at[:, own_rows], slot).astype(BF16)
        ks_ref[i % 2, i // 2] = kv

        @pl.when(core == i % 2)
        def _():
            kv_ref[chip, i // 2, own_rows] = kv
        w_start(i + DEPTH, 'kv' if i + DEPTH < n_k else 'q')
        if i == 0:
            pl.semaphore_wait(barrier, group - 1)
            x_copy.start()
        kv_sent(i, lambda cp: cp.start())
    tab_own.start()
    for cp in tab_copies:
        cp.start()

    def kv_part(c, g, b, to):
        ref = kv_ref.at[c, g, pl.ds(b * rows, rows)]
        return remote(ref, ref, kvf_sem.at[g, b], kvr_sem.at[c, g, b], lane(to))

    def kv_wait(c, g):
        kv_part(c, g, 0, right).wait_recv()
        kv_part(c, g, 1, right).wait_recv()

    def kv_passed(g, act):
        c, to = (left, right) if g < n_kv // 2 else (right, left)

        @pl.when(to > c)
        def _():
            for b in range(2):
                act(kv_part(c, g, b, to))

    def kv_relay(g):
        low = low_head(g)
        pl.when(to_right(left, low))(lambda: kv_wait(left, g))
        pl.when(to_left(right, low))(lambda: kv_wait(right, g))
        kv_passed(g, lambda cp: cp.start())

    x_copy.wait_recv()
    x_copy.wait_send()
    def w_next(i):
        nxt = i + DEPTH
        lap = (nxt - n_k) // half

        @pl.when((nxt < n_w) & (lax.rem(lap, 2) == 0))
        def _():
            w_start(nxt, 'q')

        @pl.when((nxt < n_w) & (lax.rem(lap, 2) == 1))
        def _():
            w_start(nxt, 'o')

    def queries(r, lo, n):
        @pl.loop(lo, lo + n)
        def _(j):
            i = n_k + 2 * r * half + j
            slot = w_wait(i, 'q')
            q_ref[j] = product(xs_ref.at[:, r * rows:(r + 1) * rows], slot).astype(BF16)
            w_next(i)

    span = half // n_kv
    for part in range(n_kv):
        queries(0, part * span, span)
        if part < n_kv - 1:
            kv_relay(part)

    n_h = 2 * per
    hb = n_h // 2
    m_rows = hb * rows

    def blk(g, r, c, size, diag):
        k_blk = kv_ref[c, g, :size, :HEAD]
        v_blk = kv_ref[c, g, :size, HEAD:]
        scores = []
        for u in range(2):
            q_u = jnp.concatenate([q_ref[g * per + (u * hb + i) // 2, :, ((u * hb + i) % 2) * HEAD:((u * hb + i) % 2 + 1) * HEAD] for i in range(hb)], axis=0)
            scores.append(lax.dot_general(q_u, k_blk, (((1,), (1,)), ((), ())), preferred_element_type=F32))
        for u in range(2):
            s = scores[u]
            if diag:
                a = lax.broadcasted_iota(jnp.int32, (rows, size), 0) + r * rows
                b = lax.broadcasted_iota(jnp.int32, (rows, size), 1)
                s = s + jnp.concatenate([jnp.where(a >= b, 0.0, NEG)] * hb, axis=0)
            cols = [s[:, b * HEAD:(b + 1) * HEAD] for b in range(size // HEAD)]
            mx = functools.reduce(jnp.maximum, cols)
            mx = jnp.broadcast_to(jnp.max(mx, axis=1, keepdims=True), (m_rows, HEAD))
            if not diag:
                m_old = m_ref[g, u]
                mx = jnp.maximum(m_old, mx)
            ps = [jnp.exp2((y - mx) * LOG_SCALE) for y in cols]
            l = functools.reduce(jnp.add, ps)
            pv = jnp.dot(jnp.concatenate([p.astype(BF16) for p in ps], axis=1), v_blk, preferred_element_type=F32)
            if not diag:
                a = jnp.exp2((m_old - mx) * LOG_SCALE)
                l = l + l_ref[g, u] * a
                pv = pv + acc_ref[g, u] * a
            m_ref[g, u] = mx
            l_ref[g, u] = l
            acc_ref[g, u] = pv

    def finish(g, r):
        for u in range(2):
            o = (acc_ref[g, u] / jnp.sum(l_ref[g, u], axis=1, keepdims=True)).astype(BF16)
            for i in range(hb):
                h = u * hb + i
                o_ref[r, mine + g * per + h // 2, :, (h % 2) * HEAD:(h % 2 + 1) * HEAD] = o[i * rows:(i + 1) * rows]

    def o_copy(r, g):
        part = o_ref.at[r, pl.ds(mine + g * per, per)]
        return remote(part, part, os_sem.at[r, g], or_sem.at[r, g], {'sp': sib})

    def o_in(r, g):
        part = o_ref.at[r, pl.ds(half - mine + g * per, per)]
        return remote(part, part, os_sem.at[r, g], or_sem.at[r, g], {'sp': sib})

    def piece(s, j):
        return h_ref.at[pl.ds(pl.multiple_of(s * rows, rows), rows), pl.ds(pl.multiple_of(j * CW, CW), CW)]

    def h_own(r, j, k, dev):
        s = chip * 2 + r
        return remote(hs_ref.at[r, j], piece(s, mine + j), hs_sem.at[k, r, j], hr_sem.at[s, mine + j], dev)

    def h_own3(r, j):
        return (h_own(r, j, 0, lane(right)), h_own(r, j, 1, lane(left)), h_own(r, j, 2, {'sp': sib}))

    def h_keep(r, j):
        return pltpu.make_async_copy(hs_ref.at[r, j], piece(chip * 2 + r, mine + j), hs_sem.at[3, r, j])

    def project(r):
        @pl.loop(0, half)
        def _(j):
            i = n_k + (1 + 2 * r) * half + j
            slot = w_wait(i, 'o')
            y = product(o_ref.at[r], slot)
            hs_ref[r, j] = (xs_ref[mine + j, r * rows:(r + 1) * rows].astype(F32) + y).astype(BF16)

            w_next(i)
            for cp in h_own3(r, j):
                cp.start()
            h_keep(r, j).start()

    first = lax.rem(chip + 1, 2)
    second = first + 2
    early = chip < chips // 2

    def h_fwd(c, r, k, j):
        ref = piece(c * 2 + r, mine + j)
        return remote(ref, ref, hf_sem.at[k, r, j], hr_sem.at[c * 2 + r, mine + j], {'sp': sib})

    def h_relay(c, to, r, k, j):
        ref = piece(c * 2 + r, mine + j)
        return remote(ref, ref, hrel_sem.at[k, r, j], hr_sem.at[c * 2 + r, mine + j], lane(to))

    cut = half * SHARE // 12

    def relayed(j):
        return early == (j < cut)

    def relay(k, r):
        c, to = ((first, second), (second, first))[k]

        @pl.loop(0, half)
        def _(j):
            h_fwd(c, r, k, j).wait_recv()

            @pl.when(relayed(j))
            def _():
                h_relay(c, to, r, k, j).start()
            h_fwd(c, r, k, j).start()

    late, last = chip >= chips // 2, chip == chips - 1
    for r in range(2):
        if r == 1:
            queries(1, 0, half)

        @pl.loop(0, n_kv)
        def _(g):
            if r == 0:
                pl.when(g == 1)(lambda: kv_relay(n_kv - 1))
                kv_part(chip, g, 1 - core, right).wait_recv()
            else:
                pl.when((g == 2) & late)(lambda: relay(0, 0))
                pl.when((g == 3) & last)(lambda: relay(1, 0))
            blk(g, r, chip, (r + 1) * rows, True)

            @pl.loop(0, 2)
            def _(n):
                c = n * right + (1 - n) * left

                @pl.when(c < chip)
                def _():
                    blk(g, r, c, 2 * rows, False)

        @pl.loop(0, n_kv)
        def _(g):
            @pl.when(opp < chip)
            def _():
                if r == 0:
                    kv_wait(opp, g)
                blk(g, r, opp, 2 * rows, False)
            finish(g, r)
            o_copy(r, g).start()
        for g in range(n_kv):
            o_in(r, g).wait_recv()
        project(r)

    pl.when(jnp.logical_not(late))(lambda: relay(0, 0))
    pl.when(jnp.logical_not(last))(lambda: relay(1, 0))
    relay(0, 1)
    relay(1, 1)
    for r in range(2):
        @pl.loop(0, half)
        def _(j):
            h_fwd(opp, r, 2, j).wait_recv()
            h_fwd(opp, r, 2, j).start()

    def from_sib(c, r, j):
        ref = piece(c * 2 + r, half - mine + j)
        return remote(ref, ref, hs_sem.at[0, r, j], hr_sem.at[c * 2 + r, half - mine + j], {'sp': sib})

    for r in range(2):
        @pl.loop(0, half)
        def _(j):
            for c in range(chips):
                from_sib(c, r, j).wait_recv()
            for cp in h_own3(r, j):
                cp.wait_send()
            h_keep(r, j).wait()
            for k, c in enumerate((first, second, opp)):
                h_fwd(c, r, k, j).wait_send()

            @pl.when(relayed(j))
            def _():
                h_relay(first, second, r, 0, j).wait_send()
                h_relay(second, first, r, 1, j).wait_send()
    for i in range(n_k):
        kv_sent(i, lambda cp: cp.wait_send())
    for g in range(n_kv):
        kv_passed(g, lambda cp: cp.wait_send())
        for b in range(2):
            o_copy(b, g).wait_send()
    tab_own.wait()
    for cp in tab_copies:
        cp.wait()


def route_kernel(group, tab_ref, h_ref, buf_ref, out_ref, in_ref, st_ref, in_sem, st_sem, own_sem):
    me = lax.axis_index('sp')
    rows, width = out_ref.shape
    experts = tab_ref.shape[1] - 8
    exp_row = lax.broadcasted_iota(jnp.int32, (experts, rows), 0)
    a = lax.broadcasted_iota(jnp.int32, (rows, rows), 0)
    b = lax.broadcasted_iota(jnp.int32, (rows, rows), 1)
    before = jnp.where(a < b, 1.0, 0.0).astype(BF16)

    def fetch(s):
        return pltpu.make_async_copy(h_ref.at[pl.ds(s * rows, rows)], in_ref.at[s], in_sem.at[s])

    def put(s):
        return pltpu.make_async_copy(st_ref.at[s % SLOTS], buf_ref.at[pl.ds(s * rows, rows)], st_sem.at[s])

    own = pltpu.make_async_copy(in_ref.at[me], out_ref, own_sem)
    for s in range(AHEAD):
        fetch(s).start()
    for s in range(group):
        tab = tab_ref[s]
        ids = tab[:2].astype(jnp.int32)
        probs = tab[8:]
        hit = jnp.max(jnp.where(ids == me, 1.0, 0.0), axis=0, keepdims=True)
        both = jnp.where((exp_row == ids[0:1]) | (exp_row == ids[1:2]), probs, 0.0)
        p_me = jnp.sum(jnp.where(exp_row == me, probs, 0.0), axis=0, keepdims=True)
        gate = p_me * hit / jnp.sum(both, axis=0, keepdims=True)
        slot = jnp.dot(jnp.broadcast_to(hit, (8, rows)).astype(BF16), before, preferred_element_type=F32)[:1].astype(jnp.int32)
        pick = (a == slot) & (hit > 0.5)
        g_slot = jnp.broadcast_to(jnp.sum(jnp.where(pick, gate, 0.0), axis=1, keepdims=True), (rows, CW))
        pick = jnp.where(pick, 1.0, 0.0).astype(BF16)
        fetch(s).wait()
        if s + AHEAD < group:
            fetch(s + AHEAD).start()
        if s >= SLOTS:
            put(s - SLOTS).wait()
        for j in range(width // CW):
            cols = slice(j * CW, (j + 1) * CW)
            got = jnp.dot(pick, in_ref[s, :, cols], preferred_element_type=F32)
            st_ref[s % SLOTS, :, cols] = (g_slot * got).astype(BF16)
        put(s).start()
    own.start()
    for s in range(group - SLOTS, group):
        put(s).wait()
    own.wait()


def solution(mesh):
    group = mesh.shape['sp']
    row_spec = P(('dp', 'sp'), None)
    buf_spec = P(('dp', 'sp'), None, None)

    def step(x, w_q, w_k, w_v, w_o, ids, probs):
        rows, width = x.shape
        experts = probs.shape[1]
        chips = group // 2
        n_col = width // CW
        half = n_col // 2
        n_kv = w_k.shape[1] // HEAD // 2
        per = half // n_kv
        crow = 2 * rows
        tab = jnp.concatenate([ids.T.astype(F32), jnp.zeros((6, rows), F32), probs.T], axis=0)
        dma = pltpu.SemaphoreType.DMA
        hbm = pl.BlockSpec(memory_space=pl.ANY)
        vm = pl.BlockSpec(memory_space=pltpu.VMEM)
        h_all, tabs = pl.pallas_call(
            functools.partial(block_kernel, group),
            in_specs=[hbm] * 5 + [vm],
            out_specs=[hbm, hbm],
            out_shape=[
                jax.ShapeDtypeStruct((group * rows, width), BF16),
                jax.ShapeDtypeStruct((group, tab.shape[0], rows), F32),
            ],
            scratch_shapes=[
                pltpu.VMEM((n_col, crow, CW), BF16),
                pltpu.VMEM((half, rows, CW), BF16),
                pltpu.VMEM((2, n_col, rows, CW), BF16),
                pltpu.VMEM((2, n_kv, rows, CW), BF16),
                pltpu.VMEM((chips, n_kv, crow, CW), BF16),
                pltpu.VMEM((DEPTH, width, CW), BF16),
                pltpu.VMEM((2, half, rows, CW), BF16),
                pltpu.VMEM((n_kv, 2, per * rows, HEAD), F32),
                pltpu.VMEM((n_kv, 2, per * rows, HEAD), F32),
                pltpu.VMEM((n_kv, 2, per * rows, HEAD), F32),
                dma((DEPTH, 2)), dma((n_col,)), dma, dma,
                dma((3, 2 * n_kv)), dma((chips, n_kv, 2)), dma((n_kv, 2)), dma((2, n_kv)), dma((2, n_kv)),
                dma((4, 2, half)), dma((3, 2, half)), dma((2, 2, half)), dma((group, n_col)),
                dma((group,)), dma((group,)),
            ],
            compiler_params=pltpu.CompilerParams(collective_id=0, has_side_effects=True, vmem_limit_bytes=56 * 1024 * 1024),
        )(x, w_q, w_k, w_v, w_o, tab)
        buf, hidden_out = pl.pallas_call(
            functools.partial(route_kernel, group),
            in_specs=[vm, hbm],
            out_specs=[hbm, hbm],
            out_shape=[jax.ShapeDtypeStruct((group * rows, width), BF16), jax.ShapeDtypeStruct((rows, width), BF16)],
            scratch_shapes=[
                pltpu.VMEM((group, rows, width), BF16),
                pltpu.VMEM((SLOTS, rows, width), BF16),
                dma((group,)), dma((group,)), dma,
            ],
            compiler_params=pltpu.CompilerParams(vmem_limit_bytes=56 * 1024 * 1024),
        )(tabs, h_all)
        return hidden_out, buf[None]

    return jax.shard_map(step, mesh=mesh, in_specs=(row_spec, P(), P(), P(), P(), row_spec, row_spec), out_specs=(row_spec, buf_spec), check_vma=False)
```
